32 devices in a mesh: batch: 2 (over x), ctx: 4 (over z), seq: 4 (over y, core).
Axes of the slice: x: 2, y: 2, z: 4, core: 2. Of those that a mesh axis runs over, the one named last changes fastest.
Arguments:
- hidden: bfloat16 [32, 6144], P('batch'), parts along dimension 0
- lengths: int32 [32], P('batch'), parts along dimension 0
- latent_cache: bfloat16 [32, 8192, 512], P('batch', ('ctx', 'seq')), parts along dimension 0
- rope_keys: bfloat16 [32, 8192, 64], P('batch', ('ctx', 'seq')), parts along dimension 0
- w_uq: bfloat16 [6144, 64, 128], P(None, 'seq')
- w_qr: bfloat16 [6144, 64, 64], P(None, 'seq')
- w_uk: bfloat16 [64, 128, 512], P('seq')
- w_uv: bfloat16 [64, 512, 128], P('seq')
- w_out: bfloat16 [64, 128, 6144], P('seq')
Outputs:
- output: bfloat16 [32, 6144], P('batch'), parts along dimension 0
There are 2 independent parts. The reference program is written for one: setup_inputs(seed, part) draws one part's arguments, and reference() takes and returns one part's arrays. A program takes and returns all parts, laid end to end along the dimension named above; an argument that names none is the same for every part.
All inputs are finite; a program needn't handle non-finite values.
Results may differ from the reference program's by a relative error of at most 0.00548613.
Values are sent between devices in bfloat16 or wider.
A program may use at most 1 GiB of HBM per device.

```python
import jax
import jax.numpy as jnp
from jax import lax

NUM_ROWS = 16
SEQ_LEN = 8192
D_MODEL = 6144
NUM_HEADS = 64
LATENT = 512
ROPE_DIM = 64
NOPE_DIM = 128
VALUE_DIM = 128
NUM_WAVES = 3

SCORE_SCALE = (NOPE_DIM + ROPE_DIM) ** -0.5
SHORT_LEN = SEQ_LEN // 8
LONG_LEN = SEQ_LEN - SEQ_LEN // 8


def wave_basis():
    spots = (jnp.arange(SEQ_LEN, dtype=jnp.float32) + 0.5) / SEQ_LEN
    waves = jnp.arange(1, NUM_WAVES + 1, dtype=jnp.float32)
    return jnp.cos(jnp.pi * spots[:, None] * waves[None, :])


def draw_rows(row_keys, width, amplitude, profile):
    def one_row(row_key):
        coef_key, noise_key = jax.random.split(row_key)
        coeffs = amplitude * jax.random.normal(coef_key, (NUM_WAVES, width), jnp.float32)
        noise = jax.random.normal(noise_key, (SEQ_LEN, width), jnp.float32)
        return (0.6 * noise + jnp.dot(profile, coeffs)).astype(jnp.bfloat16)
    return lax.map(one_row, row_keys)


def draw_lengths(len_key):
    coin_key, long_key, short_key = jax.random.split(len_key, 3)
    coins = jax.random.randint(coin_key, (NUM_ROWS,), 0, 2)
    long_lens = jax.random.randint(long_key, (NUM_ROWS,), LONG_LEN, SEQ_LEN + 1)
    short_lens = jax.random.randint(short_key, (NUM_ROWS,), SHORT_LEN, SEQ_LEN + 1)
    lengths = jnp.where(coins == 1, long_lens, short_lens)
    return lengths.at[0].set(SEQ_LEN).at[1].set(SHORT_LEN).astype(jnp.int32)


def setup_inputs(seed: int = 0, part: int = 0) -> dict:
    base_key = jax.random.key(seed)
    part_key = jax.random.fold_in(base_key, part)
    weight_keys = jax.random.split(base_key, 5)
    data_keys = jax.random.split(part_key, 4)
    profile = wave_basis()
    q_scale = 0.6 * D_MODEL ** -0.5
    hidden = jax.random.normal(data_keys[0], (NUM_ROWS, D_MODEL), jnp.float32)
    w_uq = q_scale * jax.random.normal(weight_keys[0], (D_MODEL, NUM_HEADS, NOPE_DIM), jnp.float32)
    w_qr = q_scale * jax.random.normal(weight_keys[1], (D_MODEL, NUM_HEADS, ROPE_DIM), jnp.float32)
    w_uk = NOPE_DIM ** -0.5 * jax.random.normal(weight_keys[2], (NUM_HEADS, NOPE_DIM, LATENT), jnp.float32)
    w_uv = LATENT ** -0.5 * jax.random.normal(weight_keys[3], (NUM_HEADS, LATENT, VALUE_DIM), jnp.float32)
    w_out = (NUM_HEADS * VALUE_DIM) ** -0.5 * jax.random.normal(weight_keys[4], (NUM_HEADS, VALUE_DIM, D_MODEL), jnp.float32)
    return {
        'hidden': hidden.astype(jnp.bfloat16),
        'lengths': draw_lengths(data_keys[1]),
        'latent_cache': draw_rows(jax.random.split(data_keys[2], NUM_ROWS), LATENT, 1.0, profile),
        'rope_keys': draw_rows(jax.random.split(data_keys[3], NUM_ROWS), ROPE_DIM, 2.0, profile),
        'w_uq': w_uq.astype(jnp.bfloat16),
        'w_qr': w_qr.astype(jnp.bfloat16),
        'w_uk': w_uk.astype(jnp.bfloat16),
        'w_uv': w_uv.astype(jnp.bfloat16),
        'w_out': w_out.astype(jnp.bfloat16),
    }


def reference(hidden, lengths, latent_cache, rope_keys, w_uq, w_qr, w_uk, w_uv, w_out):
    q_nope = jnp.dot(hidden, w_uq.reshape(D_MODEL, NUM_HEADS * NOPE_DIM), preferred_element_type=jnp.float32)
    q_nope = q_nope.astype(jnp.bfloat16).reshape(NUM_ROWS, NUM_HEADS, NOPE_DIM)
    q_rope = jnp.dot(hidden, w_qr.reshape(D_MODEL, NUM_HEADS * ROPE_DIM), preferred_element_type=jnp.float32)
    q_rope = q_rope.astype(jnp.bfloat16).reshape(NUM_ROWS, NUM_HEADS, ROPE_DIM)
    q_lat = jnp.einsum('bhk,hkc->bhc', q_nope.astype(jnp.float32), w_uk.astype(jnp.float32)).astype(jnp.bfloat16)
    positions = jnp.arange(SEQ_LEN)

    def one_row(row_data):
        lat_row, rope_row, cache_row, keys_row, length = row_data
        scores = jnp.dot(lat_row, cache_row.T, preferred_element_type=jnp.float32)
        scores = (scores + jnp.dot(rope_row, keys_row.T, preferred_element_type=jnp.float32)) * SCORE_SCALE
        valid = positions[None, :] < length
        scores = jnp.where(valid, scores, -jnp.inf)
        row_max = jnp.max(scores, axis=1, keepdims=True)
        weights = jnp.exp(scores - row_max)
        weight_sum = jnp.sum(weights, axis=1, keepdims=True)
        weighted = jnp.dot(weights.astype(jnp.bfloat16), cache_row, preferred_element_type=jnp.float32)
        return (weighted / weight_sum).astype(jnp.bfloat16)

    lat_out = lax.map(one_row, (q_lat, q_rope, latent_cache, rope_keys, lengths))
    head_vals = jnp.einsum('bhc,hcv->bhv', lat_out.astype(jnp.float32), w_uv.astype(jnp.float32)).astype(jnp.bfloat16)
    mixed = jnp.einsum('bhv,hvd->bd', head_vals.astype(jnp.float32), w_out.astype(jnp.float32))
    return (hidden.astype(jnp.float32) + mixed).astype(jnp.bfloat16)
```

```python
import functools

import jax
import jax.numpy as jnp
from jax import lax
from jax.experimental import pallas as pl
from jax.experimental.pallas import tpu as pltpu
from jax.sharding import PartitionSpec as P

MESH = pl.DeviceIdType.MESH
F32, BF16 = jnp.float32, jnp.bfloat16
NEG = -3.0e38

ROWS, D, HLOC, NOPE, ROPE, LAT, VAL = 16, 6144, 16, 128, 64, 512, 128
TLOC = 512
QW = LAT + 128
CH = 768
NCH = D // CH
SLOTS = 4
HALF = D // 2


def mm(a, b):
    return lax.dot_general(a, b, (((1,), (0,)), ((), ())), preferred_element_type=F32)


def mm_nt(a, b):
    return lax.dot_general(a, b, (((1,), (1,)), ((), ())), preferred_element_type=F32)


def onehot(shape, fn):
    i = lax.broadcasted_iota(jnp.int32, shape, 0)
    j = lax.broadcasted_iota(jnp.int32, shape, 1)
    return jnp.where(fn(i, j), 1.0, 0.0).astype(BF16)


def merge(a, mla, b, mlb):
    ma, mb = mla[:, 0:1], mlb[:, 0:1]
    m = jnp.maximum(ma, mb)
    fa, fb = jnp.exp(ma - m), jnp.exp(mb - m)
    l = mla[:, 1:2] * fa + mlb[:, 1:2] * fb
    return a * fa + b * fb, pack_ml(m, l)


def pack_ml(m, l):
    lane = lax.broadcasted_iota(jnp.int32, (m.shape[0], 128), 1)
    return jnp.where(lane == 0, m, jnp.where(lane == 1, l, 0.0))


def kernel(len_ref, hid_hbm, cache_hbm, rope_hbm, wuq_hbm, wqr_hbm, wuk_hbm, wuv_hbm, wout_hbm, out_ref,
           hid, cache, rope, wuq, wqr, wuk, wuv, wout, rep, qall, qb, acc, ml, racc, rml, ysa, ysm, yra, yrm,
           zsa, zsm, zra, zrm, yb, yr, tr, fin, hsel, outf,
           lsem, usem, csem, bar_unused, ag_s, ag_r, d_s, d_r, y_s, y_r, z_s, z_r, f_s, f_r):
    x = lax.axis_index("batch")
    z = lax.axis_index("ctx")
    s = lax.axis_index("seq")
    y, k = s // 2, s % 2
    sp = s + 1 - 2 * k
    sy = s + 2 - 4 * y
    zx = {1: z + 1 - 2 * (z % 2), 2: z + 2 - 4 * (z // 2), 3: 3 - z}

    dev_p, dev_y = (x, z, sp), (x, z, sy)
    dev_z = {j: (x, zx[j], s) for j in zx}
    peers = [dev_p, dev_y, dev_z[1], dev_z[2], dev_z[3]]

    barrier = pltpu.get_barrier_semaphore()
    for d in peers:
        pl.semaphore_signal(barrier, inc=1, device_id=d, device_id_type=MESH)

    def local(src, dst, sem):
        c = pltpu.make_async_copy(src, dst, sem)
        c.start()
        return c

    def remote(src, dst, ss, rs, dev):
        return pltpu.make_async_remote_copy(src_ref=src, dst_ref=dst, send_sem=ss, recv_sem=rs,
                                            device_id=dev, device_id_type=MESH)

    c_hid = local(hid_hbm, hid, lsem.at[0])
    hh = pl.multiple_of(8 * (z // 2), 8)

    def uq_copy(i, slot):
        return pltpu.make_async_copy(wuq_hbm.at[pl.ds(pl.multiple_of(i * CH, CH), CH), pl.ds(hh, 8), :],
                                     wuq.at[slot], usem.at[slot])

    for i in range(SLOTS):
        uq_copy(i, i).start()
    c_qr = local(wqr_hbm.at[pl.ds(4 * z, 4)], wqr, lsem.at[1])
    c_uk = local(wuk_hbm.at[pl.ds(4 * z, 4)], wuk, lsem.at[2])

    spread = onehot((128, 1024), lambda i, j: j // 8 == i)
    c_hid.wait()

    for t in range(6):
        blk = jnp.concatenate([hid[:, (8 * t + i) * 128:(8 * t + i + 1) * 128] for i in range(8)], axis=0)
        rep[pl.ds(8 * t, 8)] = mm(blk, spread).astype(BF16).reshape(8, 16, 1024)

    lane = lax.broadcasted_iota(jnp.int32, (16, 128), 1)
    masks = [jnp.where(lane % 8 == 4 * (z % 2) + h, 1.0, 0.0).astype(BF16) for h in range(4)]
    wide = [jnp.concatenate([m] * (CH * 8 // 128), axis=1) for m in masks]

    def chunk(i, qn):
        slot = lax.rem(i, SLOTS)
        uq_copy(i, slot).wait()
        r = jnp.concatenate([rep[i * 6 + t] for t in range(6)], axis=1)
        lhs = jnp.concatenate([r * m for m in wide], axis=0)
        qn = qn + mm(lhs, wuq[slot].reshape(CH * 8, NOPE))

        @pl.when(i + SLOTS < NCH)
        def _():
            uq_copy(i + SLOTS, slot).start()
        return qn

    qn = lax.fori_loop(0, NCH, chunk, jnp.zeros((64, NOPE), F32)).astype(BF16)

    c_rope = local(rope_hbm, rope, lsem.at[3])
    c_cache = [local(cache_hbm.at[pl.ds(4 * g, 4)], cache.at[pl.ds(4 * g, 4)], csem.at[g]) for g in range(4)]
    c_uv = local(wuv_hbm, wuv, lsem.at[4])
    c_out = local(wout_hbm, wout, lsem.at[5])

    c_qr.wait()
    qr = mm_nt(hid[...], wqr[...].reshape(4 * ROPE, D)).astype(BF16)
    c_uk.wait()
    parts = []
    for h in range(4):
        ql = mm(qn[16 * h:16 * h + 16], wuk[h]).astype(BF16)
        rr = jnp.concatenate([qr[:, ROPE * h:ROPE * h + ROPE], jnp.zeros((16, 64), BF16)], axis=1)
        parts.append(jnp.concatenate([ql, rr], axis=1))
    q = jnp.concatenate(parts, axis=0)
    turn = onehot((64, 64), lambda i, j: (i % 4) * 16 + i // 4 == j)
    me = s * 4 + z
    qall[me] = mm(turn, q).astype(BF16)

    pl.semaphore_wait(barrier, len(peers))
    sends = []

    def send(piece, sem_i, dev):
        c = remote(qall.at[piece], qall.at[piece], ag_s.at[sem_i], ag_r.at[piece], dev)
        c.start()
        sends.append(c)

    def arrived(piece):
        remote(qall.at[piece], qall.at[piece], ag_s.at[0], ag_r.at[piece], dev_p).wait_recv()

    send(me, 0, dev_y)
    for n, j in enumerate((1, 2, 3)):
        send(me, 1 + n, dev_z[j])
    send(me, 4, dev_p)
    ns = 5
    for j in (1, 2, 3):
        pz = s * 4 + zx[j]
        arrived(pz)
        send(pz, ns, dev_y)
        send(pz, ns + 1, dev_p)
        ns += 2
    for zz in (z, zx[1], zx[2], zx[3]):
        py = sy * 4 + zz
        arrived(py)
        send(py, ns, dev_p)
        ns += 1

    pick = onehot((16, 16), lambda i, j: 4 * z + i == j)
    hsel[...] = mm(pick, hid[...])[0:4]

    for ss in (sp, sp + 2 - 4 * y):
        for zz in (z, zx[1], zx[2], zx[3]):
            arrived(ss * 4 + zz)
    for c in sends:
        c.wait_send()

    perm = onehot((256, 256), lambda i, j: ((i % 64) // 4) * 16 + (i // 64) * 4 + i % 4 == j)
    scale = (NOPE + ROPE) ** -0.5
    t0 = (z * 4 + s) * TLOC
    c_rope.wait()
    for c in c_cache:
        c.wait()

    def attend(g):
        rows = pl.ds(pl.multiple_of(16 * g, 16), 16)
        xg = jnp.concatenate([qall[p, rows, :] for p in range(16)], axis=0)
        qb[...] = mm(perm, xg).astype(BF16).reshape(4, 64, QW)

        def row(i, carry):
            b = 4 * g + i
            q = qb[i]
            kv = cache[b]
            sc = mm_nt(q[:, :LAT], kv) + mm(q[:, LAT:LAT + ROPE], rope[b])
            sc = sc * scale
            valid = lax.broadcasted_iota(jnp.int32, (64, TLOC), 1) < len_ref[b] - t0
            sc = jnp.where(valid, sc, NEG)
            m = jnp.max(sc, axis=1, keepdims=True)
            w = jnp.where(valid, jnp.exp(sc - m), 0.0)
            l = jnp.sum(w, axis=1, keepdims=True)
            acc[b] = mm(w.astype(BF16), kv).reshape(4, 16, LAT)
            ml[b] = pack_ml(m, l).reshape(4, 16, 128)
            return carry

        lax.fori_loop(0, 4, row, 0)

    def d_copies(j, g):
        out = []
        for n in range(2):
            so = 2 * n + (1 - k)
            rows = pl.ds(4 * g, 4)
            out.append(remote(acc.at[rows, so], racc.at[j, n], d_s.at[j, 2 * n], d_r.at[j, 2 * n], dev_p))
            out.append(remote(ml.at[rows, so], rml.at[j, n], d_s.at[j, 2 * n + 1], d_r.at[j, 2 * n + 1], dev_p))
        return out

    def y_copies(j):
        return [remote(ysa.at[j], yra.at[j], y_s.at[j, 0], y_r.at[j, 0], dev_y),
                remote(ysm.at[j], yrm.at[j], y_s.at[j, 1], y_r.at[j, 1], dev_y)]

    def z_copies(j):
        return [remote(zsa.at[j], zra.at[j], z_s.at[j, 0], z_r.at[j, 0], dev_z[j]),
                remote(zsm.at[j], zrm.at[j], z_s.at[j, 1], z_r.at[j, 1], dev_z[j])]

    order = (3, 2, 1, 0)
    gs = {0: z, **zx}

    def stage_d(j):
        attend(gs[j])
        for c in d_copies(j, gs[j]):
            c.start()

    def stage_y(j):
        for c in d_copies(j, gs[j]):
            c.wait_recv()
        for n in range(2):
            so = 2 * n + k

            def piece(i, carry):
                b = 4 * gs[j] + i
                a, q = merge(acc[b, so], ml[b, so], racc[j, n, i], rml[j, n, i])
                acc[b, so] = a
                ml[b, so] = q
                return carry
            lax.fori_loop(0, 4, piece, 0)

        def give(i, carry):
            ysa[j, i] = acc[4 * gs[j] + i, 2 * (1 - y) + k]
            ysm[j, i] = ml[4 * gs[j] + i, 2 * (1 - y) + k]
            return carry
        lax.fori_loop(0, 4, give, 0)
        for c in y_copies(j):
            c.start()

    def stage_z(j):
        for c in y_copies(j):
            c.wait_recv()

        def piece(i, carry):
            b = 4 * gs[j] + i
            a, q = merge(acc[b, s], ml[b, s], yra[j, i], yrm[j, i])
            zsa[j, i] = a
            zsm[j, i] = q
            return carry
        lax.fori_loop(0, 4, piece, 0)
        if j:
            for c in z_copies(j):
                c.start()

    for n in range(len(order) + 2):
        if n < 4:
            stage_d(order[n])
        if 0 <= n - 1 < 4:
            stage_y(order[n - 1])
        if 0 <= n - 2 < 4:
            stage_z(order[n - 2])

    for j in (1, 2, 3):
        for c in z_copies(j):
            c.wait_recv()
    ol = []
    for i in range(4):
        a, q = zsa[0, i], zsm[0, i]
        for j in (1, 2, 3):
            a, q = merge(a, q, zra[j, i], zrm[j, i])
        ol.append((a / q[:, 1:2]).astype(BF16))
    ol = jnp.concatenate(ol, axis=0)

    c_uv.wait()
    vs = []
    head = lax.broadcasted_iota(jnp.int32, (64, VAL), 0) % 16
    for h in range(HLOC):
        v = mm(ol, wuv[h])
        vs.append(jnp.where(head == h, v, 0.0).astype(BF16))
    v = jnp.concatenate(vs, axis=1)
    fold = onehot((16, 64), lambda i, j: j // 16 == i)
    v = mm(fold, v).astype(BF16)

    c_out.wait()
    w = 768
    for n in range(2):
        def cols(i, carry):
            at = pl.multiple_of(n * HALF + i * w, w)
            r = mm(v, wout[:, :, pl.ds(at, w)].reshape(HLOC * VAL, w))
            yb[n, :, pl.ds(pl.multiple_of(i * w, w), w)] = r[0:4]
            return carry
        lax.fori_loop(0, HALF // w, cols, 0)

    c = remote(yb, yr, f_s.at[0], f_r.at[0], dev_p)
    c.start()
    c.wait_recv()
    tr[0] = yb[k] + yr[k]
    cy = remote(tr.at[0], tr.at[1], f_s.at[1], f_r.at[1], dev_y)
    cy.start()
    cy.wait_recv()
    res = hsel[:, pl.ds(pl.multiple_of(k * HALF, HALF), HALF)] + (tr[0] + tr[1])
    fin[z, k] = res.astype(BF16)

    last = [remote(fin.at[z, k], fin.at[z, k], f_s.at[2], f_r.at[2], dev_p)]
    for j in (1, 2, 3):
        last.append(remote(fin.at[z, k], fin.at[z, k], f_s.at[2 + j], f_r.at[2 + j], dev_z[j]))
    for d in last:
        d.start()
    for j in (1, 2, 3):
        remote(fin.at[zx[j], k], fin.at[zx[j], k], f_s.at[2 + j], f_r.at[2 + j], dev_z[j]).wait_recv()
        d = remote(fin.at[zx[j], k], fin.at[zx[j], k], f_s.at[5 + j], f_r.at[5 + j], dev_p)
        d.start()
        last.append(d)
    remote(fin.at[z, 1 - k], fin.at[z, 1 - k], f_s.at[2], f_r.at[2], dev_p).wait_recv()
    for j in (1, 2, 3):
        remote(fin.at[zx[j], 1 - k], fin.at[zx[j], 1 - k], f_s.at[5 + j], f_r.at[5 + j], dev_p).wait_recv()
    for i in range(4):
        for n in range(2):
            outf[4 * i:4 * i + 4, n * HALF:(n + 1) * HALF] = fin[i, n].astype(F32)
    out_ref[...] = outf[...].astype(BF16)

    for j in order:
        for d in d_copies(j, gs[j]) + y_copies(j) + (z_copies(j) if j else []):
            d.wait_send()
    for d in [c, cy] + last:
        d.wait_send()


def solution(mesh):
    def local_step(hidden, lengths, latent_cache, rope_keys, w_uq, w_qr, w_uk, w_uv, w_out):
        rope_t = jnp.transpose(rope_keys, (0, 2, 1))
        wqr_t = jnp.transpose(w_qr, (1, 2, 0))
        anyspec = pl.BlockSpec(memory_space=pl.ANY)
        dma = pltpu.SemaphoreType.DMA
        scratch = [
            pltpu.VMEM((ROWS, D), BF16),
            pltpu.VMEM((ROWS, TLOC, LAT), BF16),
            pltpu.VMEM((ROWS, ROPE, TLOC), BF16),
            pltpu.VMEM((SLOTS, CH, 8, NOPE), BF16),
            pltpu.VMEM((4, ROPE, D), BF16),
            pltpu.VMEM((4, NOPE, LAT), BF16),
            pltpu.VMEM((HLOC, LAT, VAL), BF16),
            pltpu.VMEM((HLOC, VAL, D), BF16),
            pltpu.VMEM((48, 16, 1024), BF16),
            pltpu.VMEM((16, 64, QW), BF16),
            pltpu.VMEM((4, 64, QW), BF16),
            pltpu.VMEM((ROWS, 4, 16, LAT), F32),
            pltpu.VMEM((ROWS, 4, 16, 128), F32),
            pltpu.VMEM((4, 2, 4, 16, LAT), F32),
            pltpu.VMEM((4, 2, 4, 16, 128), F32),
            pltpu.VMEM((4, 4, 16, LAT), F32),
            pltpu.VMEM((4, 4, 16, 128), F32),
            pltpu.VMEM((4, 4, 16, LAT), F32),
            pltpu.VMEM((4, 4, 16, 128), F32),
            pltpu.VMEM((4, 4, 16, LAT), F32),
            pltpu.VMEM((4, 4, 16, 128), F32),
            pltpu.VMEM((4, 4, 16, LAT), F32),
            pltpu.VMEM((4, 4, 16, 128), F32),
            pltpu.VMEM((2, 4, HALF), F32),
            pltpu.VMEM((2, 4, HALF), F32),
            pltpu.VMEM((2, 4, HALF), F32),
            pltpu.VMEM((4, 2, 4, HALF), BF16),
            pltpu.VMEM((4, D), F32),
            pltpu.VMEM((ROWS, D), F32),
            dma((6,)), dma((SLOTS,)), dma((4,)), dma((1,)),
            dma((15,)), dma((16,)),
            dma((4, 4)), dma((4, 4)),
            dma((4, 2)), dma((4, 2)),
            dma((4, 2)), dma((4, 2)),
            dma((9,)), dma((9,)),
        ]
        return pl.pallas_call(
            kernel,
            out_shape=jax.ShapeDtypeStruct((ROWS, D), BF16),
            in_specs=[pl.BlockSpec(memory_space=pltpu.SMEM)] + [anyspec] * 8,
            out_specs=pl.BlockSpec(memory_space=pltpu.VMEM),
            scratch_shapes=scratch,
            compiler_params=pltpu.CompilerParams(collective_id=0, has_side_effects=True,
                                                 vmem_limit_bytes=67_000_000),
        )(lengths, hidden, latent_cache, rope_t, w_uq, wqr_t, w_uk, w_uv, w_out)

    row_spec, cache_spec = P('batch', None), P('batch', ('ctx', 'seq'), None)
    head_spec, proj_spec = P('seq', None, None), P(None, 'seq', None)
    return jax.shard_map(local_step, mesh=mesh,
                         in_specs=(row_spec, P('batch'), cache_spec, cache_spec, proj_spec, proj_spec, head_spec, head_spec, head_spec),
                         out_specs=row_spec, check_vma=False)
```

```python
import functools

import jax
import jax.numpy as jnp
from jax import lax
from jax.experimental import pallas as pl
from jax.experimental.pallas import tpu as pltpu
from jax.sharding import PartitionSpec as P

MESH = pl.DeviceIdType.MESH
F32, BF16 = jnp.float32, jnp.bfloat16
NEG = -3.0e38

ROWS, D, HLOC, NOPE, ROPE, LAT, VAL = 16, 6144, 16, 128, 64, 512, 128
TLOC = 512
QW = LAT + 128
CH = 1536
NCH = D // CH
BLK = CH // 128
QUART = D // 4


def mm(a, b):
    return lax.dot_general(a, b, (((1,), (0,)), ((), ())), preferred_element_type=F32)


def mm_nt(a, b):
    return lax.dot_general(a, b, (((1,), (1,)), ((), ())), preferred_element_type=F32)


def onehot(shape, fn):
    i = lax.broadcasted_iota(jnp.int32, shape, 0)
    j = lax.broadcasted_iota(jnp.int32, shape, 1)
    return jnp.where(fn(i, j), 1.0, 0.0).astype(BF16)


def put(ml, i, m, l):
    lane = lax.broadcasted_iota(jnp.int32, ml.shape, 1)
    return jnp.where(lane == i, m, jnp.where(lane == 4 + i, l, ml))


def merge4(parts, mls):
    out, ml = [], jnp.zeros((16, 128), F32)
    for i in range(4):
        ms = [q[:, i:i + 1] for q in mls]
        m = functools.reduce(jnp.maximum, ms)
        fs = [jnp.exp(v - m) for v in ms]
        l = functools.reduce(jnp.add, [q[:, 4 + i:5 + i] * f for q, f in zip(mls, fs)])
        out.append(functools.reduce(jnp.add, [p(i) * f for p, f in zip(parts, fs)]))
        ml = put(ml, i, m, l)
    return out, ml


def kernel(len_ref, hid_hbm, cache_hbm, rope_hbm, wuq_hbm, wqr_hbm, wuk_hbm, wuv_hbm, wout_hbm, out_ref,
           hid, cache, rope, wuq, wqr, wuk, wuv, wout, rep, zq, qnb, qg, acc, ml, racc, rml,
           yra, yrm, zra, zrm, yb, yr, tr, fin, hsel, outf,
           lsem, usem, csem, q_s, q_r, a_s, a_r, d_s, d_r, y_s, y_r, z_s, z_r, e_s, e_r, t_s, t_r, f_s, f_r):
    x = lax.axis_index("batch")
    z = lax.axis_index("ctx")
    s = lax.axis_index("seq")
    y, k = s // 2, s % 2
    sp = s + 1 - 2 * k
    sy = s + 2 - 4 * y
    spy = sp + 2 - 4 * y
    zx = {1: z + 1 - 2 * (z % 2), 2: z + 2 - 4 * (z // 2), 3: 3 - z}
    gs = {0: z, **zx}
    order = (3, 2, 1, 0)

    dev_p, dev_y = (x, z, sp), (x, z, sy)
    dev_z = {j: (x, zx[j], s) for j in zx}
    peers = [dev_p, dev_y, dev_z[1], dev_z[2], dev_z[3]]

    barrier = pltpu.get_barrier_semaphore()
    for d in peers:
        pl.semaphore_signal(barrier, inc=1, device_id=d, device_id_type=MESH)

    def local(src, dst, sem):
        c = pltpu.make_async_copy(src, dst, sem)
        c.start()
        return c

    def remote(src, dst, ss, rs, dev):
        return pltpu.make_async_remote_copy(src_ref=src, dst_ref=dst, send_sem=ss, recv_sem=rs,
                                            device_id=dev, device_id_type=MESH)

    started = []

    def go(c):
        c.start()
        started.append(c)

    own4 = pl.ds(pl.multiple_of(4 * z, 4), 4)
    c_hid = local(hid_hbm, hid, lsem.at[0])

    def load_uq(i):
        return local(wuq_hbm.at[pl.ds(i * CH, CH), own4, :], wuq.at[i], usem.at[i])

    c_uq = [load_uq(0), load_uq(1)]
    c_qr = local(wqr_hbm.at[own4], wqr, lsem.at[1])
    c_uq += [load_uq(2), load_uq(3)]
    c_uk = local(wuk_hbm, wuk, lsem.at[2])

    spread = onehot((128, 512), lambda i, j: j // 4 == i)
    lane = lax.broadcasted_iota(jnp.int32, (16, 128), 1)
    masks = [jnp.where(lane % 4 == h, 1.0, 0.0).astype(BF16) for h in range(4)]
    wide = [jnp.concatenate([m] * (CH * 4 // 128), axis=1) for m in masks]
    c_hid.wait()
    for t in range(NCH):
        blk = jnp.concatenate([hid[:, (BLK * t + i) * 128:(BLK * t + i + 1) * 128] for i in range(BLK)], axis=0)
        rep[pl.ds(BLK * t, BLK)] = mm(blk, spread).astype(BF16).reshape(BLK, 16, 512)
    qn = jnp.zeros((64, NOPE), F32)
    for i in range(NCH):
        c_uq[i].wait()
        r = jnp.concatenate([rep[i * BLK + t] for t in range(BLK)], axis=1)
        lhs = jnp.concatenate([r * m for m in wide], axis=0)
        qn = qn + mm(lhs, wuq[i].reshape(CH * 4, NOPE))
        if i == 1:
            c_qr.wait()
            qr = mm_nt(hid[...], wqr[...].reshape(4 * ROPE, D)).astype(BF16)
    qn = qn.astype(BF16)
    rr = jnp.concatenate([qr[:, ROPE * h:ROPE * h + ROPE] for h in range(4)], axis=0)
    zq[z] = jnp.concatenate([qn, rr, jnp.zeros((64, 64), BF16)], axis=1)
    c_rope = local(rope_hbm, rope, lsem.at[3])
    c_cache = {j: local(cache_hbm.at[pl.ds(4 * gs[j], 4)], cache.at[pl.ds(4 * gs[j], 4)], csem.at[j]) for j in order}
    c_uv = local(wuv_hbm, wuv, lsem.at[4])
    c_out = local(wout_hbm, wout, lsem.at[5])

    pl.semaphore_wait(barrier, len(peers))
    for j in (3, 2, 1):
        go(remote(zq.at[z], zq.at[z], q_s.at[j - 1], q_r.at[z], dev_z[j]))
    pick = onehot((16, 16), lambda i, j: 4 * z + i == j)
    hsel[...] = mm(pick, hid[...])[0:4]
    perm = onehot((256, 256), lambda i, j: (i % 16) * 16 + i // 16 == j)
    row16 = lax.broadcasted_iota(jnp.int32, (16, 128), 0)
    hm = [jnp.concatenate([jnp.where(row16 == h, 1.0, 0.0).astype(BF16)] * 4, axis=0) for h in range(HLOC)]
    for j in (1, 2, 3):
        remote(zq.at[zx[j]], zq.at[zx[j]], q_s.at[0], q_r.at[zx[j]], dev_p).wait_recv()
    qnb[...] = mm(perm, zq[...].reshape(256, 256)).astype(BF16).reshape(4, 64, 256)
    c_uk.wait()

    for j in order:
        qb = qnb[gs[j]]
        lhs = jnp.concatenate([qb[:, :NOPE] * hm[h] for h in range(HLOC)], axis=1)
        ql = mm(lhs, wuk[...].reshape(HLOC * NOPE, LAT)).astype(BF16)
        qg[j, s] = jnp.concatenate([ql, qb[:, NOPE:]], axis=1)
        go(remote(qg.at[j, s], qg.at[j, s], a_s.at[j, 0], a_r.at[j, s], dev_y))
        go(remote(qg.at[j, s], qg.at[j, s], a_s.at[j, 1], a_r.at[j, s], dev_p))

    def arrived(j, who):
        remote(qg.at[j, who], qg.at[j, who], a_s.at[j, 0], a_r.at[j, who], dev_p).wait_recv()

    def forward(j):
        arrived(j, sy)
        go(remote(qg.at[j, sy], qg.at[j, sy], a_s.at[j, 2], a_r.at[j, sy], dev_p))

    scale = (NOPE + ROPE) ** -0.5
    t0 = (z * 4 + s) * TLOC

    def attend(j, rows, mlv):
        sc, ws = [], []
        for i in rows:
            b = 4 * gs[j] + i
            q = jnp.concatenate([qg[j, p, 16 * i:16 * i + 16, :] for p in range(4)], axis=0)
            sc.append(mm_nt(q[:, :LAT], cache[b]) + mm(q[:, LAT:LAT + ROPE], rope[b]))
        for n, i in enumerate(rows):
            b = 4 * gs[j] + i
            valid = lax.broadcasted_iota(jnp.int32, (64, TLOC), 1) < len_ref[b] - t0
            v = jnp.where(valid, sc[n] * scale, NEG)
            m = jnp.max(v, axis=1, keepdims=True)
            w = jnp.where(valid, jnp.exp(v - m), 0.0)
            mlv = put(mlv, i, m, jnp.sum(w, axis=1, keepdims=True))
            ws.append(w.astype(BF16))
        for n, i in enumerate(rows):
            o = mm(ws[n], cache[4 * gs[j] + i])
            for p in range(4):
                acc[j, p, i] = o[16 * p:16 * p + 16]
        return mlv

    def d_copies(j):
        out = []
        for n in range(2):
            so = 2 * n + (1 - k)
            out.append(remote(acc.at[j, so], racc.at[j, n], d_s.at[j, 2 * n], d_r.at[j, 2 * n], dev_p))
            out.append(remote(ml.at[j, so], rml.at[j, n], d_s.at[j, 2 * n + 1], d_r.at[j, 2 * n + 1], dev_p))
        return out

    def y_copies(j):
        so = 2 * (1 - y) + k
        return [remote(acc.at[j, so], yra.at[j], y_s.at[j, 0], y_r.at[j, 0], dev_y),
                remote(ml.at[j, so], yrm.at[j], y_s.at[j, 1], y_r.at[j, 1], dev_y)]

    def z_copies(j):
        return [remote(acc.at[j, s], zra.at[j], z_s.at[j, 0], z_r.at[j, 0], dev_z[j]),
                remote(ml.at[j, s], zrm.at[j], z_s.at[j, 1], z_r.at[j, 1], dev_z[j])]

    def add(j, so, ra, rm):
        out, q = merge4([lambda i: acc[j, so, i], ra], [ml[j, so], rm])
        for i in range(4):
            acc[j, so, i] = out[i]
        ml[j, so] = q

    def stage_y(j):
        for c in d_copies(j):
            c.wait_recv()
        add(j, 2 * (1 - y) + k, lambda i: racc[j, 1 - y, i], rml[j, 1 - y])
        for c in y_copies(j):
            go(c)
        add(j, s, lambda i: racc[j, y, i], rml[j, y])

    def stage_z(j):
        for c in y_copies(j):
            c.wait_recv()
        add(j, s, lambda i: yra[j, i], yrm[j])
        if j:
            for c in z_copies(j):
                go(c)

    forward(order[0])
    c_rope.wait()
    for n in range(len(order) + 2):
        if n < 4:
            j = order[n]
            arrived(j, sp)
            arrived(j, spy)
            c_cache[j].wait()
            mlv = attend(j, (0, 1), jnp.zeros((64, 128), F32))
            if n < 3:
                forward(order[n + 1])
            mlv = attend(j, (2, 3), mlv)
            ml[j] = mlv.reshape(4, 16, 128)
            for c in d_copies(j):
                go(c)
        if 0 <= n - 1 < 4:
            stage_y(order[n - 1])
        if 0 <= n - 2 < 4:
            stage_z(order[n - 2])

    for j in (1, 2, 3):
        for c in z_copies(j):
            c.wait_recv()
    c_uv.wait()
    c_out.wait()
    out, q = merge4([lambda i: acc[0, s, i]] + [functools.partial(lambda j, i: zra[j, i], j) for j in (1, 2, 3)],
                    [ml[0, s], zrm[1], zrm[2], zrm[3]])
    ol = jnp.concatenate([(out[i] / q[:, 4 + i:5 + i]).astype(BF16) for i in range(4)], axis=0)
    vs = []
    head = lax.broadcasted_iota(jnp.int32, (64, VAL), 0) % 16
    for h in range(HLOC):
        vs.append(jnp.where(head == h, mm(ol, wuv[h]), 0.0).astype(BF16))
    v = jnp.concatenate(vs, axis=1)
    fold = onehot((16, 64), lambda i, j: j // 16 == i)
    v = mm(fold, v).astype(BF16)

    def cols(c):
        at = pl.multiple_of(c * QUART, QUART)
        return mm(v, wout[:, :, pl.ds(at, QUART)].reshape(HLOC * VAL, QUART))[0:4]

    def e_copy(n):
        return remote(yb.at[n], yr.at[n], e_s.at[n], e_r.at[n], dev_p)

    def t_copy(n):
        return remote(tr.at[0, n], tr.at[1, n], t_s.at[n], t_r.at[n], dev_y)

    def finish(n):
        t_copy(n).wait_recv()
        c = 2 * k + n
        res = hsel[:, pl.ds(pl.multiple_of(c * QUART, QUART), QUART)] + (tr[0, n] + tr[1, n])
        fin[z, c] = res.astype(BF16)
        for j in (3, 2, 1):
            go(remote(fin.at[z, c], fin.at[z, c], f_s.at[n, j], f_r.at[n, j], dev_z[j]))
        go(remote(fin.at[z, c], fin.at[z, c], f_s.at[n, 0], f_r.at[n, 0], dev_p))

    for n in range(2):
        yb[n] = cols(2 * (1 - k) + n)
        go(e_copy(n))
    for n in range(2):
        part = cols(2 * k + n)
        e_copy(n).wait_recv()
        tr[0, n] = part + yr[n]
        go(t_copy(n))
        if n:
            finish(0)
    finish(1)
    for n in range(2):
        for j in (1, 2, 3):
            at = fin.at[zx[j], 2 * k + n]
            remote(at, at, f_s.at[n, 0], f_r.at[n, j], dev_p).wait_recv()
            go(remote(at, at, f_s.at[n, 3 + j], f_r.at[n, 3 + j], dev_p))
    for n in range(2):
        for j in range(4):
            at = fin.at[gs[j], 2 * (1 - k) + n]
            remote(at, at, f_s.at[n, 0], f_r.at[n, 3 + j if j else 0], dev_p).wait_recv()
    for i in range(4):
        for c in range(4):
            outf[4 * i:4 * i + 4, c * QUART:(c + 1) * QUART] = fin[i, c].astype(F32)
    out_ref[...] = outf[...].astype(BF16)
    for c in started:
        c.wait_send()


def solution(mesh):
    def local_step(hidden, lengths, latent_cache, rope_keys, w_uq, w_qr, w_uk, w_uv, w_out):
        rope_t = jnp.transpose(rope_keys, (0, 2, 1))
        wqr_t = jnp.transpose(w_qr, (1, 2, 0))
        anyspec = pl.BlockSpec(memory_space=pl.ANY)
        dma = pltpu.SemaphoreType.DMA
        scratch = [
            pltpu.VMEM((ROWS, D), BF16),
            pltpu.VMEM((ROWS, TLOC, LAT), BF16),
            pltpu.VMEM((ROWS, ROPE, TLOC), BF16),
            pltpu.VMEM((NCH, CH, 4, NOPE), BF16),
            pltpu.VMEM((4, ROPE, D), BF16),
            pltpu.VMEM((HLOC, NOPE, LAT), BF16),
            pltpu.VMEM((HLOC, LAT, VAL), BF16),
            pltpu.VMEM((HLOC, VAL, D), BF16),
            pltpu.VMEM((48, 16, 512), BF16),
            pltpu.VMEM((4, 64, 256), BF16),
            pltpu.VMEM((4, 64, 256), BF16),
            pltpu.VMEM((4, 4, 64, QW), BF16),
            pltpu.VMEM((4, 4, 4, 16, LAT), F32),
            pltpu.VMEM((4, 4, 16, 128), F32),
            pltpu.VMEM((4, 2, 4, 16, LAT), F32),
            pltpu.VMEM((4, 2, 16, 128), F32),
        ]
        for _ in range(2):
            scratch += [pltpu.VMEM((4, 4, 16, LAT), F32), pltpu.VMEM((4, 16, 128), F32)]
        scratch += [
            pltpu.VMEM((2, 4, QUART), F32),
            pltpu.VMEM((2, 4, QUART), F32),
            pltpu.VMEM((2, 2, 4, QUART), F32),
            pltpu.VMEM((4, 4, 4, QUART), BF16),
            pltpu.VMEM((4, D), F32),
            pltpu.VMEM((ROWS, D), F32),
            dma((6,)), dma((NCH,)), dma((4,)),
            dma((3,)), dma((4,)),
            dma((4, 3)), dma((4, 4)),
            dma((4, 4)), dma((4, 4)),
            dma((4, 2)), dma((4, 2)),
            dma((4, 2)), dma((4, 2)),
            dma((2,)), dma((2,)), dma((2,)), dma((2,)),
            dma((2, 7)), dma((2, 7)),
        ]
        return pl.pallas_call(
            kernel,
            out_shape=pltpu.VMEM((ROWS, D), BF16),
            in_specs=[pl.BlockSpec(memory_space=pltpu.SMEM)] + [anyspec] * 8,
            out_specs=pl.BlockSpec(memory_space=pltpu.VMEM),
            scratch_shapes=scratch,
            compiler_params=pltpu.CompilerParams(collective_id=0, has_side_effects=True,
                                                 vmem_limit_bytes=66_000_000),
        )(lengths, hidden, latent_cache, rope_t, w_uq, wqr_t, w_uk, w_uv, w_out)

    row_spec, cache_spec = P('batch', None), P('batch', ('ctx', 'seq'), None)
    head_spec, proj_spec = P('seq', None, None), P(None, 'seq', None)
    return jax.shard_map(local_step, mesh=mesh,
                         in_specs=(row_spec, P('batch'), cache_spec, cache_spec, proj_spec, proj_spec, head_spec, head_spec, head_spec),
                         out_specs=row_spec, check_vma=False)
```

```python
import functools

import jax
import jax.numpy as jnp
from jax import lax
from jax.experimental import pallas as pl
from jax.experimental.pallas import tpu as pltpu
from jax.sharding import PartitionSpec as P

MESH = pl.DeviceIdType.MESH
F32, BF16 = jnp.float32, jnp.bfloat16
NEG = -3.0e38

ROWS, D, HLOC, NOPE, ROPE, LAT, VAL = 16, 6144, 16, 128, 64, 512, 128
TLOC = 512
QW = LAT + 128
CH = 1536
NCH = D // CH
BLK = CH // 128
QUART = D // 4


def mm(a, b):
    return lax.dot_general(a, b, (((1,), (0,)), ((), ())), preferred_element_type=F32)


def mm_nt(a, b):
    return lax.dot_general(a, b, (((1,), (1,)), ((), ())), preferred_element_type=F32)


def onehot(shape, fn):
    i = lax.broadcasted_iota(jnp.int32, shape, 0)
    j = lax.broadcasted_iota(jnp.int32, shape, 1)
    return jnp.where(fn(i, j), 1.0, 0.0).astype(BF16)


def pack(ms, ls):
    lane = lax.broadcasted_iota(jnp.int32, (8, 128), 1)
    t = jnp.zeros((8, 128), F32)
    for i in range(2):
        for at, v in ((i, ms[i][0:8]), (2 + i, ms[i][8:16]), (4 + i, ls[i][0:8]), (6 + i, ls[i][8:16])):
            t = jnp.where(lane == at, v, t)
    return t


def unpack(t, i):
    return [jnp.concatenate([t[:, at + i:at + i + 1], t[:, at + 2 + i:at + 3 + i]], axis=0) for at in (0, 4)]


def merge(parts, tiles):
    out, nm, nl = [], [], []
    for i in range(2):
        mls = [unpack(t, i) for t in tiles]
        m = functools.reduce(jnp.maximum, [v[0] for v in mls])
        fs = [jnp.exp(v[0] - m) for v in mls]
        nl.append(functools.reduce(jnp.add, [v[1] * f for v, f in zip(mls, fs)]))
        nm.append(m)
        out.append(functools.reduce(jnp.add, [p(i) * f for p, f in zip(parts, fs)]))
    return out, nm, nl


def kernel(len_ref, hid_hbm, cache_hbm, rope_hbm, wuq_hbm, wqr_hbm, wuk_hbm, wuv_hbm, wout_hbm, out_ref,
           hid, cache, rope, wuq, wqr, wuk, wuv, wout, rep, zq, xq, qg, acc, ml, racc, rml, yra, yrm, zra, zrm,
           yb, yr, tr, fin, hsel, outf,
           lsem, usem, csem, q_s, q_r, a_s, a_r, d_s, d_r, y_s, y_r, z_s, z_r, e_s, e_r, t_s, t_r, f_s, f_r):
    x = lax.axis_index("batch")
    z = lax.axis_index("ctx")
    s = lax.axis_index("seq")
    y, k = s // 2, s % 2
    sp = s + 1 - 2 * k
    sy = s + 2 - 4 * y
    spy = sp + 2 - 4 * y
    zx = {1: z + 1 - 2 * (z % 2), 2: z + 2 - 4 * (z // 2), 3: 3 - z}
    inner = ((z + 1) // 2) % 2
    gs = [3 * (1 - z // 2), 2 - z // 2, zx[1], z]

    dev_p, dev_y = (x, z, sp), (x, z, sy)
    dev_z = {j: (x, zx[j], s) for j in zx}
    peers = [dev_p, dev_y, dev_z[1], dev_z[2], dev_z[3]]

    def local(src, dst, sem):
        c = pltpu.make_async_copy(src, dst, sem)
        c.start()
        return c

    def remote(src, dst, ss, rs, dev):
        return pltpu.make_async_remote_copy(src_ref=src, dst_ref=dst, send_sem=ss, recv_sem=rs,
                                            device_id=dev, device_id_type=MESH)

    started = []

    def go(c):
        c.start()
        started.append(c)

    own4 = pl.ds(pl.multiple_of(4 * z, 4), 4)
    c_hid = local(hid_hbm, hid, lsem.at[0])

    def load_uq(i):
        return local(wuq_hbm.at[pl.ds(i * CH, CH), own4, :], wuq.at[i], usem.at[i])

    c_qr = local(wqr_hbm.at[own4], wqr, lsem.at[1])
    c_uq = [load_uq(i) for i in range(NCH)]
    c_uk = local(wuk_hbm, wuk, lsem.at[2])

    barrier = pltpu.get_barrier_semaphore()
    for d in peers:
        pl.semaphore_signal(barrier, inc=1, device_id=d, device_id_type=MESH)

    spread = onehot((128, 512), lambda i, j: j // 4 == i)
    lane = lax.broadcasted_iota(jnp.int32, (16, 128), 1)
    masks = [jnp.where(lane % 4 == h, 1.0, 0.0).astype(BF16) for h in range(4)]
    wide = [jnp.concatenate([m] * (CH * 4 // 128), axis=1) for m in masks]
    c_hid.wait()
    for t in range(NCH):
        blk = jnp.concatenate([hid[:, (BLK * t + i) * 128:(BLK * t + i + 1) * 128] for i in range(BLK)], axis=0)
        rep[pl.ds(BLK * t, BLK)] = mm(blk, spread).astype(BF16).reshape(BLK, 16, 512)
    c_qr.wait()
    half = D // 2
    qr = (mm_nt(hid[:, :half], wqr[:, :, :half].reshape(4 * ROPE, half))
          + mm_nt(hid[:, half:], wqr[:, :, half:].reshape(4 * ROPE, half))).astype(BF16)
    zq[z, 64:80] = qr[:, :128]
    zq[z, 80:96] = qr[:, 128:]
    qn = jnp.zeros((64, NOPE), F32)
    for i in range(NCH):
        c_uq[i].wait()
        r = jnp.concatenate([rep[i * BLK + t] for t in range(BLK)], axis=1)
        lhs = jnp.concatenate([r * m for m in wide], axis=0)
        qn = qn + mm(lhs, wuq[i].reshape(CH * 4, NOPE))
    zq[z, 0:64] = qn.astype(BF16)
    c_rope = local(rope_hbm, rope, lsem.at[3])
    c_cache = [local(cache_hbm.at[pl.ds(4 * g, 4)], cache.at[pl.ds(4 * g, 4)], csem.at[n]) for n, g in enumerate(gs)]
    c_uv = local(wuv_hbm, wuv, lsem.at[4])
    c_out = local(wout_hbm, wout, lsem.at[5])

    pl.semaphore_wait(barrier, len(peers))
    for j in (3, 2, 1):
        go(remote(zq.at[z], zq.at[z], q_s.at[j - 1], q_r.at[z], dev_z[j]))
    pick = onehot((16, 16), lambda i, j: 4 * z + i == j)
    hsel[...] = mm(pick, hid[...])[0:4]

    def row_of(i):
        return sum((jnp.where(i // 4 == n, 4 * g, 0) for n, g in enumerate(gs))) + i % 4

    perm = onehot((256, 256), lambda i, j: (i % 16) * 16 + row_of(i // 16) == j)

    def latent(zz):
        for h in range(4):
            ql = mm(zq[zz, 16 * h:16 * h + 16], wuk[4 * zz + h]).astype(BF16)
            t = zq[zz, 64 + 16 * (h // 2):80 + 16 * (h // 2)]
            if h % 2:
                t = jnp.concatenate([t[:, 64:], t[:, :64]], axis=1)
            xq[4 * zz + h] = jnp.concatenate([ql, t], axis=1)

    c_uk.wait()
    latent(z)
    for j in (1, 2, 3):
        remote(zq.at[zx[j]], zq.at[zx[j]], q_s.at[0], q_r.at[zx[j]], dev_p).wait_recv()
        latent(zx[j])
    qp = mm(perm, xq[...].reshape(256, QW)).astype(BF16)
    for u in range(8):
        qg[u, s] = qp[32 * u:32 * u + 32]
    for u in range(8):
        go(remote(qg.at[u, s], qg.at[u, s], a_s.at[u, 0], a_r.at[u, s], dev_y))
        go(remote(qg.at[u, s], qg.at[u, s], a_s.at[u, 1], a_r.at[u, s], dev_p))

    def arrived(u, who):
        remote(qg.at[u, who], qg.at[u, who], a_s.at[u, 0], a_r.at[u, who], dev_p).wait_recv()

    def forward(u):
        arrived(u, sy)
        go(remote(qg.at[u, sy], qg.at[u, sy], a_s.at[u, 2], a_r.at[u, sy], dev_p))

    scale = (NOPE + ROPE) ** -0.5
    t0 = (z * 4 + s) * TLOC

    def attend(u):
        bs = [4 * gs[u // 2] + 2 * (u % 2) + i for i in range(2)]
        sc, ws, ms, ls = [], [], [], []
        for i, b in enumerate(bs):
            q = jnp.concatenate([qg[u, p, 16 * i:16 * i + 16, :] for p in range(4)], axis=0)
            sc.append(mm_nt(q[:, :LAT], cache[b]) + mm(q[:, LAT:LAT + ROPE], rope[b]))
        for i, b in enumerate(bs):
            valid = lax.broadcasted_iota(jnp.int32, (64, TLOC), 1) < len_ref[b] - t0
            v = jnp.where(valid, sc[i] * scale, NEG)
            m = jnp.max(v, axis=1, keepdims=True)
            w = jnp.where(valid, jnp.exp(v - m), 0.0)
            ms.append(m)
            ls.append(jnp.sum(w, axis=1, keepdims=True))
            ws.append(w.astype(BF16))
        for i, b in enumerate(bs):
            o = mm(ws[i], cache[b])
            for p in range(4):
                acc[u, p % 2, p // 2, i] = o[16 * p:16 * p + 16]
        for p in range(4):
            cut = slice(16 * p, 16 * p + 16)
            ml[u, p % 2, p // 2] = pack([m[cut] for m in ms], [l[cut] for l in ls])

    def d_copies(u):
        return [remote(acc.at[u, 1 - k], racc.at[u], d_s.at[u, 0], d_r.at[u, 0], dev_p),
                remote(ml.at[u, 1 - k], rml.at[u], d_s.at[u, 1], d_r.at[u, 1], dev_p)]

    def y_copies(u):
        return [remote(acc.at[u, k, 1 - y], yra.at[u], y_s.at[u, 0], y_r.at[u, 0], dev_y),
                remote(ml.at[u, k, 1 - y], yrm.at[u], y_s.at[u, 1], y_r.at[u, 1], dev_y)]

    def z_copies(u):
        n, h = u // 2, u % 2
        to = zx[1] if n == 2 else inner * gs[n] + (1 - inner) * zx[1]
        at = 2 if n == 2 else inner * 3 + (1 - inner) * n
        return [remote(acc.at[u, k, y], zra.at[at, h], z_s.at[u, 0], z_r.at[at, h, 0], (x, to, s)),
                remote(ml.at[u, k, y], zrm.at[at, h], z_s.at[u, 1], z_r.at[at, h, 1], (x, to, s))]

    def z_wait(at, h):
        remote(zra.at[at, h], zra.at[at, h], z_s.at[0, 0], z_r.at[at, h, 0], dev_p).wait_recv()
        remote(zrm.at[at, h], zrm.at[at, h], z_s.at[0, 1], z_r.at[at, h, 1], dev_p).wait_recv()

    def add(u, yy, ra, rm):
        out, m, l = merge([lambda i: acc[u, k, yy, i], ra], [ml[u, k, yy], rm])
        for i in range(2):
            acc[u, k, yy, i] = out[i]
        ml[u, k, yy] = pack(m, l)

    def stage_a(u):
        arrived(u, sp)
        arrived(u, spy)
        if u < 7:
            forward(u + 1)
        if u % 2 == 0:
            c_cache[u // 2].wait()
        attend(u)
        for c in d_copies(u):
            go(c)

    def stage_y(u):
        for c in d_copies(u):
            c.wait_recv()
        add(u, 1 - y, lambda i: racc[u, 1 - y, i], rml[u, 1 - y])
        for c in y_copies(u):
            go(c)
        add(u, y, lambda i: racc[u, y, i], rml[u, y])

    def stage_z(u):
        for c in y_copies(u):
            c.wait_recv()
        add(u, y, lambda i: yra[u, i], yrm[u])
        if u < 4:
            @pl.when(inner == 0)
            def _():
                for c in z_copies(u):
                    c.start()
        elif u < 6:
            for c in z_copies(u):
                go(c)

    def stage_c(u):
        @pl.when(inner == 1)
        def _():
            n, h = u // 2, u % 2
            z_wait(n, h)
            add(u, y, lambda i: zra[n, h, i], zrm[n, h])
            for c in z_copies(u):
                c.start()

    forward(0)
    c_rope.wait()
    plan = []
    for u in range(8):
        ready = 1.2 * (u + 5) if u < 4 else 1.47 * u + 4.9
        plan += [(1.2 * u, stage_a, u), (1.2 * (u + 1) + 0.1, stage_y, u), (ready, stage_z, u)]
        if u < 4:
            plan.append((ready + 3.6, stage_c, u))
    for _, stage, u in sorted(plan, key=lambda e: e[0]):
        stage(u)

    for at in (2, 3):
        for h in range(2):
            z_wait(at, h)
    c_uv.wait()
    c_out.wait()
    ol = []
    for h in range(2):
        u = 6 + h
        out, m, l = merge([lambda i: acc[u, k, y, i], lambda i: zra[2, h, i], lambda i: zra[3, h, i]],
                          [ml[u, k, y], zrm[2, h], zrm[3, h]])
        ol += [(out[i] / l[i]).astype(BF16) for i in range(2)]
    ol = jnp.concatenate(ol, axis=0)
    vs = []
    head = lax.broadcasted_iota(jnp.int32, (64, VAL), 0) % 16
    for h in range(HLOC):
        vs.append(jnp.where(head == h, mm(ol, wuv[h]), 0.0).astype(BF16))
    v = jnp.concatenate(vs, axis=1)
    fold = onehot((16, 64), lambda i, j: j // 16 == i)
    v = mm(fold, v).astype(BF16)

    def cols(c):
        at = pl.multiple_of(c * QUART, QUART)
        return mm(v, wout[:, :, pl.ds(at, QUART)].reshape(HLOC * VAL, QUART))[0:4]

    def e_copy(n):
        return remote(yb.at[n], yr.at[n], e_s.at[n], e_r.at[n], dev_p)

    def t_copy(n):
        return remote(tr.at[0, n], tr.at[1, n], t_s.at[n], t_r.at[n], dev_y)

    def finish(n):
        t_copy(n).wait_recv()
        c = 2 * k + n
        res = hsel[:, pl.ds(pl.multiple_of(c * QUART, QUART), QUART)] + (tr[0, n] + tr[1, n])
        fin[z, c] = res.astype(BF16)
        for j in (3, 2, 1):
            go(remote(fin.at[z, c], fin.at[z, c], f_s.at[n, j], f_r.at[n, j], dev_z[j]))
        go(remote(fin.at[z, c], fin.at[z, c], f_s.at[n, 0], f_r.at[n, 0], dev_p))

    for n in range(2):
        yb[n] = cols(2 * (1 - k) + n)
        go(e_copy(n))
    for n in range(2):
        part = cols(2 * k + n)
        e_copy(n).wait_recv()
        tr[0, n] = part + yr[n]
        go(t_copy(n))
        if n:
            finish(0)
    finish(1)
    for n in range(2):
        for j in (1, 2, 3):
            at = fin.at[zx[j], 2 * k + n]
            remote(at, at, f_s.at[n, 0], f_r.at[n, j], dev_p).wait_recv()
            go(remote(at, at, f_s.at[n, 3 + j], f_r.at[n, 3 + j], dev_p))
    for n in range(2):
        for j, zz in enumerate((z, zx[1], zx[2], zx[3])):
            at = fin.at[zz, 2 * (1 - k) + n]
            remote(at, at, f_s.at[n, 0], f_r.at[n, 3 + j if j else 0], dev_p).wait_recv()
    for i in range(4):
        for c in range(4):
            outf[4 * i:4 * i + 4, c * QUART:(c + 1) * QUART] = fin[i, c].astype(F32)
    out_ref[...] = outf[...].astype(BF16)
    for c in started:
        c.wait_send()
    for u in range(4):
        for c in z_copies(u):
            c.wait_send()


def solution(mesh):
    def local_step(hidden, lengths, latent_cache, rope_keys, w_uq, w_qr, w_uk, w_uv, w_out):
        rope_t = jnp.transpose(rope_keys, (0, 2, 1))
        wqr_t = jnp.transpose(w_qr, (1, 2, 0))
        anyspec = pl.BlockSpec(memory_space=pl.ANY)
        dma = pltpu.SemaphoreType.DMA
        scratch = [
            pltpu.VMEM((ROWS, D), BF16),
            pltpu.VMEM((ROWS, TLOC, LAT), BF16),
            pltpu.VMEM((ROWS, ROPE, TLOC), BF16),
            pltpu.VMEM((NCH, CH, 4, NOPE), BF16),
            pltpu.VMEM((4, ROPE, D), BF16),
            pltpu.VMEM((HLOC, NOPE, LAT), BF16),
            pltpu.VMEM((HLOC, LAT, VAL), BF16),
            pltpu.VMEM((HLOC, VAL, D), BF16),
            pltpu.VMEM((48, 16, 512), BF16),
            pltpu.VMEM((4, 96, 128), BF16),
            pltpu.VMEM((HLOC, 16, QW), BF16),
            pltpu.VMEM((8, 4, 32, QW), BF16),
            pltpu.VMEM((8, 2, 2, 2, 16, LAT), F32),
            pltpu.VMEM((8, 2, 2, 8, 128), F32),
            pltpu.VMEM((8, 2, 2, 16, LAT), F32),
            pltpu.VMEM((8, 2, 8, 128), F32),
            pltpu.VMEM((8, 2, 16, LAT), F32),
            pltpu.VMEM((8, 8, 128), F32),
            pltpu.VMEM((4, 2, 2, 16, LAT), F32),
            pltpu.VMEM((4, 2, 8, 128), F32),
            pltpu.VMEM((2, 4, QUART), F32),
            pltpu.VMEM((2, 4, QUART), F32),
            pltpu.VMEM((2, 2, 4, QUART), F32),
            pltpu.VMEM((4, 4, 4, QUART), BF16),
            pltpu.VMEM((4, D), F32),
            pltpu.VMEM((ROWS, D), F32),
            dma((6,)), dma((NCH,)), dma((4,)),
            dma((3,)), dma((4,)),
            dma((8, 3)), dma((8, 4)),
            dma((8, 2)), dma((8, 2)),
            dma((8, 2)), dma((8, 2)),
            dma((8, 2)), dma((4, 2, 2)),
            dma((2,)), dma((2,)), dma((2,)), dma((2,)),
            dma((2, 7)), dma((2, 7)),
        ]
        return pl.pallas_call(
            kernel,
            out_shape=pltpu.VMEM((ROWS, D), BF16),
            in_specs=[pl.BlockSpec(memory_space=pltpu.SMEM)] + [anyspec] * 8,
            out_specs=pl.BlockSpec(memory_space=pltpu.VMEM),
            scratch_shapes=scratch,
            compiler_params=pltpu.CompilerParams(collective_id=0, has_side_effects=True,
                                                 vmem_limit_bytes=66_000_000),
        )(lengths, hidden, latent_cache, rope_t, w_uq, wqr_t, w_uk, w_uv, w_out)

    row_spec, cache_spec = P('batch', None), P('batch', ('ctx', 'seq'), None)
    head_spec, proj_spec = P('seq', None, None), P(None, 'seq', None)
    return jax.shard_map(local_step, mesh=mesh,
                         in_specs=(row_spec, P('batch'), cache_spec, cache_spec, proj_spec, proj_spec, head_spec, head_spec, head_spec),
                         out_specs=row_spec, check_vma=False)
```

```python
import functools

import jax
import jax.numpy as jnp
from jax import lax
from jax.experimental import pallas as pl
from jax.experimental.pallas import tpu as pltpu
from jax.sharding import PartitionSpec as P

MESH = pl.DeviceIdType.MESH
F32, BF16 = jnp.float32, jnp.bfloat16
NEG = -3.0e38

ROWS, D, HLOC, NOPE, ROPE, LAT, VAL = 16, 6144, 16, 128, 64, 512, 128
TLOC = 512
QW = LAT + 128
CH = 1536
NCH = D // CH
BLK = CH // 128
QUART = D // 4
PACE = 1.2


def mm(a, b):
    return lax.dot_general(a, b, (((1,), (0,)), ((), ())), preferred_element_type=F32)


def mm_nt(a, b):
    return lax.dot_general(a, b, (((1,), (1,)), ((), ())), preferred_element_type=F32)


def onehot(shape, fn):
    i = lax.broadcasted_iota(jnp.int32, shape, 0)
    j = lax.broadcasted_iota(jnp.int32, shape, 1)
    return jnp.where(fn(i, j), 1.0, 0.0).astype(BF16)


def pack(ms, ls):
    lane = lax.broadcasted_iota(jnp.int32, (8, 128), 1)
    t = jnp.zeros((8, 128), F32)
    for i in range(2):
        for at, v in ((i, ms[i][0:8]), (2 + i, ms[i][8:16]), (4 + i, ls[i][0:8]), (6 + i, ls[i][8:16])):
            t = jnp.where(lane == at, v, t)
    return t


def unpack(t, i):
    return [jnp.concatenate([t[:, at + i:at + i + 1], t[:, at + 2 + i:at + 3 + i]], axis=0) for at in (0, 4)]


def merge(refs):
    out, nm, nl = [], [], []
    tiles = [r[128:136] for r in refs]
    for i in range(2):
        mls = [unpack(t, i) for t in tiles]
        m = functools.reduce(jnp.maximum, [v[0] for v in mls])
        fs = [jnp.exp(v[0] - m) for v in mls]
        nl.append(functools.reduce(jnp.add, [v[1] * f for v, f in zip(mls, fs)]))
        nm.append(m)
        for c in range(4):
            at = 16 * (4 * i + c)
            out.append(functools.reduce(jnp.add, [r[at:at + 16] * f for r, f in zip(refs, fs)]))
    return out, nm, nl


def kernel(len_ref, hid_hbm, cache_hbm, rope_hbm, wuq_hbm, wqr_hbm, wuk_hbm, wuv_hbm, wout_hbm, out_ref,
           hid, cache, rope, wuq, wqr, wuk, wuv, wout, rep, zq, xq, qg, sbuf, acc, racc, yra, zra,
           yb, yr, tr, fin, hsel, outf,
           lsem, usem, csem, q_s, q_r, a_s, a_r, d_s, d_r, y_s, y_r, z_s, z_r, e_s, e_r, t_s, t_r, f_s, f_r):
    x = lax.axis_index("batch")
    z = lax.axis_index("ctx")
    s = lax.axis_index("seq")
    y, k = s // 2, s % 2
    sp = s + 1 - 2 * k
    sy = s + 2 - 4 * y
    spy = sp + 2 - 4 * y
    zx = {1: z + 1 - 2 * (z % 2), 2: z + 2 - 4 * (z // 2), 3: 3 - z}
    inner = ((z + 1) // 2) % 2
    gs = [3 * (1 - z // 2), 2 - z // 2, zx[1], z]

    dev_p, dev_y = (x, z, sp), (x, z, sy)
    dev_z = {j: (x, zx[j], s) for j in zx}
    peers = [dev_p, dev_y, dev_z[1], dev_z[2], dev_z[3]]

    def local(src, dst, sem, priority=1):
        c = pltpu.make_async_copy(src, dst, sem)
        c.start(priority=priority)
        return c

    def remote(src, dst, ss, rs, dev):
        return pltpu.make_async_remote_copy(src_ref=src, dst_ref=dst, send_sem=ss, recv_sem=rs,
                                            device_id=dev, device_id_type=MESH)

    def go(c):
        c.start()

    own4 = pl.ds(pl.multiple_of(4 * z, 4), 4)
    c_hid = local(hid_hbm, hid, lsem.at[0], 0)

    def load_uq(i):
        return local(wuq_hbm.at[pl.ds(i * CH, CH), own4, :], wuq.at[i], usem.at[i])

    c_uq = [load_uq(i) for i in range(NCH)]
    c_qr = local(wqr_hbm.at[own4], wqr, lsem.at[1])

    barrier = pltpu.get_barrier_semaphore()
    for d in peers:
        pl.semaphore_signal(barrier, inc=1, device_id=d, device_id_type=MESH)

    spread = onehot((128, 512), lambda i, j: j // 4 == i)
    lane = lax.broadcasted_iota(jnp.int32, (16, 128), 1)
    masks = [jnp.where(lane % 4 == h, 1.0, 0.0).astype(BF16) for h in range(4)]
    wide = [jnp.concatenate([m] * (CH * 4 // 128), axis=1) for m in masks]
    c_hid.wait()
    for t in range(NCH):
        blk = jnp.concatenate([hid[:, (BLK * t + i) * 128:(BLK * t + i + 1) * 128] for i in range(BLK)], axis=0)
        rep[pl.ds(BLK * t, BLK)] = mm(blk, spread).astype(BF16).reshape(BLK, 16, 512)
    qn = [jnp.zeros((64, NOPE), F32)] * 2
    for i in range(0, NCH, 2):
        c_uq[i].wait()
        c_uq[i + 1].wait()
        for part in range(2):
            for n in range(2):
                at, size = part * (BLK // 2), BLK // 2
                r = jnp.concatenate([rep[(i + n) * BLK + at + t] for t in range(size)], axis=1)
                lhs = jnp.concatenate([r * m[:, :size * 512] for m in wide], axis=0)
                qn[n] = qn[n] + mm(lhs, wuq[i + n, at * 128:(at + size) * 128].reshape(size * 512, NOPE))
        if i == 0:
            c_uk = local(wuk_hbm, wuk, lsem.at[2])
    c_qr.wait()
    qr = jnp.concatenate([mm_nt(hid[...], wqr[2 * h:2 * h + 2].reshape(2 * ROPE, D)) for h in range(2)], axis=1)
    qr = qr.astype(BF16)
    zq[z, 64:80] = qr[:, :128]
    zq[z, 80:96] = qr[:, 128:]
    zq[z, 0:64] = (qn[0] + qn[1]).astype(BF16)
    c_rope = local(rope_hbm, rope, lsem.at[3])
    c_cache = local(cache_hbm, cache, csem.at[0])
    c_uv = local(wuv_hbm, wuv, lsem.at[4])
    c_out = local(wout_hbm, wout, lsem.at[5])

    pl.semaphore_wait(barrier, len(peers))
    def give_z():
        for j in (3, 2, 1):
            remote(zq.at[z], zq.at[z], q_s.at[0], q_r.at[z], dev_z[j]).start()

    give_z()
    pick = onehot((16, 16), lambda i, j: 4 * z + i == j)
    hsel[...] = mm(pick, hid[...])[0:4]

    def row_of(i):
        return sum((jnp.where(i // 4 == n, 4 * g, 0) for n, g in enumerate(gs))) + i % 4

    perm = onehot((256, 256), lambda i, j: (i % 16) * 16 + row_of(i // 16) == j)

    def latent(zz):
        for h in range(4):
            ql = mm(zq[zz, 16 * h:16 * h + 16], wuk[4 * zz + h]).astype(BF16)
            t = zq[zz, 64 + 16 * (h // 2):80 + 16 * (h // 2)]
            if h % 2:
                t = jnp.concatenate([t[:, 64:], t[:, :64]], axis=1)
            xq[4 * zz + h] = jnp.concatenate([ql, t], axis=1)

    c_uk.wait()
    latent(z)
    for j in (1, 2, 3):
        remote(zq.at[zx[j]], zq.at[zx[j]], q_s.at[0], q_r.at[zx[j]], dev_p).wait_recv()
        latent(zx[j])
    qp = mm(perm, xq[...].reshape(256, QW)).astype(BF16)
    for u in range(8):
        qg[u, 0] = qp[32 * u:32 * u + 32]
        go(remote(qg.at[u, 0], qg.at[u, 1], a_s.at[0], a_r.at[u, 0], dev_y))
        go(remote(qg.at[u, 0], qg.at[u, 2], a_s.at[1], a_r.at[u, 1], dev_p))

    def arrived(u, n):
        remote(qg.at[u, n], qg.at[u, n], a_s.at[0], a_r.at[u, n - 1], dev_p).wait_recv()

    def forward(u):
        arrived(u, 1)
        go(remote(qg.at[u, 1], qg.at[u, 3], a_s.at[2], a_r.at[u, 2], dev_p))

    scale = (NOPE + ROPE) ** -0.5
    t0 = (z * 4 + s) * TLOC

    def rows_of(u):
        return [4 * gs[u // 2] + 2 * (u % 2) + i for i in range(2)]

    def scores(u):
        for i, b in enumerate(rows_of(u)):
            q = jnp.concatenate([qg[u, p, 16 * i:16 * i + 16, :] for p in range(4)], axis=0)
            sbuf[u % 2, i] = mm_nt(q[:, :LAT], cache[b]) + mm(q[:, LAT:LAT + ROPE], rope[b])

    def attend(u):
        ws, ms, ls = [], [], []
        for i, b in enumerate(rows_of(u)):
            valid = lax.broadcasted_iota(jnp.int32, (64, TLOC), 1) < len_ref[b] - t0
            v = jnp.where(valid, sbuf[u % 2, i] * scale, NEG)
            m = jnp.max(v, axis=1, keepdims=True)
            w = jnp.where(valid, jnp.exp(v - m), 0.0)
            ms.append(m)
            ls.append(jnp.sum(w, axis=1, keepdims=True))
            ws.append(w.astype(BF16))
        for i, b in enumerate(rows_of(u)):
            o = mm(ws[i], cache[b])
            for p in range(4):
                for c in range(4):
                    acc[u, p, 16 * (4 * i + c):16 * (4 * i + c) + 16] = o[16 * p:16 * p + 16, 128 * c:128 * c + 128]
        for p in range(4):
            cut = slice(16 * p, 16 * p + 16)
            acc[u, p, 128:136] = pack([m[cut] for m in ms], [l[cut] for l in ls])

    def d_copy(u):
        return remote(acc.at[u, pl.ds(2, 2)], racc.at[u], d_s.at[0], d_r.at[u], dev_p)

    def y_copy(u):
        return remote(acc.at[u, 1], yra.at[u], y_s.at[0], y_r.at[u], dev_y)

    def z_copy(u):
        n, h = u // 2, u % 2
        to = zx[1] if n == 2 else inner * gs[n] + (1 - inner) * zx[1]
        at = 2 if n == 2 else inner * 3 + (1 - inner) * n
        return remote(acc.at[u, 0], zra.at[at, h], z_s.at[0], z_r.at[at, h], (x, to, s))

    def z_wait(at, h):
        remote(zra.at[at, h], zra.at[at, h], z_s.at[0], z_r.at[at, h], dev_p).wait_recv()

    def add(u, n, other):
        out, m, l = merge([acc[u, n], other])
        for c, o in enumerate(out):
            acc[u, n, 16 * c:16 * c + 16] = o
        acc[u, n, 128:136] = pack(m, l)

    def ready(u):
        arrived(u, 2)
        arrived(u, 3)
        if u < 7:
            forward(u + 1)
        scores(u)

    def stage_r(u):
        ready(u)

    def stage_a(u):
        if 0 < u < 7:
            ready(u + 1)
        attend(u)
        go(d_copy(u))

    def stage_y(u):
        d_copy(u).wait_recv()
        add(u, 1, racc[u, 1])
        go(y_copy(u))
        add(u, 0, racc[u, 0])

    def stage_z(u):
        y_copy(u).wait_recv()
        add(u, 0, yra[u])
        if u < 4:
            @pl.when(inner == 0)
            def _():
                z_copy(u).start()
        elif u < 6:
            go(z_copy(u))

    def stage_c(u):
        @pl.when(inner == 1)
        def _():
            z_wait(u // 2, u % 2)
            add(u, 0, zra[u // 2, u % 2])
            z_copy(u).start()

    forward(0)
    c_rope.wait()
    c_cache.wait()
    plan = [(-1, stage_r, 0), (0.2, stage_r, 1)]
    for u in range(8):
        at = PACE * (u + 5) if u < 4 else 1.47 * u + 4.9
        plan += [(PACE * u, stage_a, u), (PACE * (u + 1) + (0.1 if u else -0.9), stage_y, u), (at, stage_z, u)]
        if u < 4:
            plan.append((at + 3.6, stage_c, u))
    for _, stage, u in sorted(plan, key=lambda e: e[0]):
        stage(u)

    for at in (2, 3):
        for h in range(2):
            z_wait(at, h)
    c_uv.wait()
    c_out.wait()
    ol = []
    for h in range(2):
        u = 6 + h
        out, m, l = merge([acc[u, 0], zra[2, h], zra[3, h]])
        ol += [jnp.concatenate([(out[4 * i + c] / l[i]).astype(BF16) for c in range(4)], axis=1) for i in range(2)]
    ol = jnp.concatenate(ol, axis=0)
    vs = []
    head = lax.broadcasted_iota(jnp.int32, (64, VAL), 0) % 16
    for h in range(HLOC):
        vs.append(jnp.where(head == h, mm(ol, wuv[h]), 0.0).astype(BF16))
    v = jnp.concatenate(vs, axis=1)
    fold = onehot((16, 64), lambda i, j: j // 16 == i)
    v = mm(fold, v).astype(BF16)

    def cols(c):
        return mm(v, wout[:, :, c * QUART:(c + 1) * QUART].reshape(HLOC * VAL, QUART))[0:4]

    def e_copy(c):
        return remote(yb.at[c], yr.at[c % 2], e_s.at[0], e_r.at[c % 2], dev_p)

    def t_copy(n):
        return remote(tr.at[0, n], tr.at[1, n], t_s.at[0], t_r.at[n], dev_y)

    def pair(c):
        n = c % 2
        e_copy(c).wait_recv()
        tr[0, n] = yb[c] + yr[n]
        t_copy(n).start()

    def finish(n):
        t_copy(n).wait_recv()
        c = 2 * k + n
        res = hsel[:, pl.ds(pl.multiple_of(c * QUART, QUART), QUART)] + (tr[0, n] + tr[1, n])
        fin[4 * z + c] = res.astype(BF16)
        for j in (3, 2, 1):
            go(remote(fin.at[4 * z + c], fin.at[4 * z + c], f_s.at[0], f_r.at[n, j], dev_z[j]))
        go(remote(fin.at[4 * z + c], fin.at[4 * z + c], f_s.at[0], f_r.at[n, 0], dev_p))

    for c in range(4):
        yb[c] = cols(c)
        pl.when(k == 1 - c // 2)(lambda: e_copy(c).start())
        if c == 1:
            pl.when(k == 0)(lambda: pair(0))
        elif c == 2:
            pl.when(k == 0)(lambda: pair(1))
        elif c == 3:
            pl.when(k == 1)(lambda: pair(2))
    pl.when(k == 1)(lambda: pair(3))
    for n in range(2):
        finish(n)
    for n in range(2):
        for j in (1, 2, 3):
            at = fin.at[4 * zx[j] + 2 * k + n]
            remote(at, at, f_s.at[0], f_r.at[n, j], dev_p).wait_recv()
            go(remote(at, at, f_s.at[0], f_r.at[n, 3 + j], dev_p))
    for n in range(2):
        for j, zz in enumerate((z, zx[1], zx[2], zx[3])):
            at = fin.at[4 * zz + 2 * (1 - k) + n]
            remote(at, at, f_s.at[0], f_r.at[n, 3 + j if j else 0], dev_p).wait_recv()
    for i in range(4):
        for c in range(4):
            outf[4 * i:4 * i + 4, c * QUART:(c + 1) * QUART] = fin[4 * i + c].astype(F32)
    out_ref[...] = outf[...].astype(BF16)
    for src, sem in ((zq.at[pl.ds(0, 3)], q_s.at[0]), (qg.at[:, 0], a_s.at[0]), (qg.at[:, 0], a_s.at[1]), (qg.at[:, 1], a_s.at[2]),
                     (acc.at[:, pl.ds(2, 2)], d_s.at[0]), (acc.at[:, 1], y_s.at[0]), (acc.at[pl.ds(0, 6), 0], z_s.at[0]),
                     (yb.at[pl.ds(0, 2)], e_s.at[0]), (tr.at[0], t_s.at[0]), (fin.at[pl.ds(0, 14)], f_s.at[0])):
        remote(src, src, sem, d_r.at[0], dev_p).wait_send()


def solution(mesh):
    def local_step(hidden, lengths, latent_cache, rope_keys, w_uq, w_qr, w_uk, w_uv, w_out):
        rope_t = jnp.transpose(rope_keys, (0, 2, 1))
        wqr_t = jnp.transpose(w_qr, (1, 2, 0))
        anyspec = pl.BlockSpec(memory_space=pl.ANY)
        dma = pltpu.SemaphoreType.DMA
        scratch = [
            pltpu.VMEM((ROWS, D), BF16),
            pltpu.VMEM((ROWS, TLOC, LAT), BF16),
            pltpu.VMEM((ROWS, ROPE, TLOC), BF16),
            pltpu.VMEM((NCH, CH, 4, NOPE), BF16),
            pltpu.VMEM((4, ROPE, D), BF16),
            pltpu.VMEM((HLOC, NOPE, LAT), BF16),
            pltpu.VMEM((HLOC, LAT, VAL), BF16),
            pltpu.VMEM((HLOC, VAL, D), BF16),
            pltpu.VMEM((48, 16, 512), BF16),
            pltpu.VMEM((4, 96, 128), BF16),
            pltpu.VMEM((HLOC, 16, QW), BF16),
            pltpu.VMEM((8, 4, 32, QW), BF16),
            pltpu.VMEM((2, 2, 64, TLOC), F32),
            pltpu.VMEM((8, 4, 136, 128), F32),
            pltpu.VMEM((8, 2, 136, 128), F32),
            pltpu.VMEM((8, 136, 128), F32),
            pltpu.VMEM((4, 2, 136, 128), F32),
            pltpu.VMEM((4, 4, QUART), F32),
            pltpu.VMEM((2, 4, QUART), F32),
            pltpu.VMEM((2, 2, 4, QUART), F32),
            pltpu.VMEM((16, 4, QUART), BF16),
            pltpu.VMEM((4, D), F32),
            pltpu.VMEM((ROWS, D), F32),
            dma((6,)), dma((NCH,)), dma((1,)),
            dma((1,)), dma((4,)),
            dma((3,)), dma((8, 3)),
            dma((1,)), dma((8,)),
            dma((1,)), dma((8,)),
            dma((1,)), dma((4, 2)),
            dma((1,)), dma((2,)), dma((1,)), dma((2,)),
            dma((1,)), dma((2, 7)),
        ]
        return pl.pallas_call(
            kernel,
            out_shape=pltpu.VMEM((ROWS, D), BF16),
            in_specs=[pl.BlockSpec(memory_space=pltpu.SMEM)] + [anyspec] * 8,
            out_specs=pl.BlockSpec(memory_space=pltpu.VMEM),
            scratch_shapes=scratch,
            compiler_params=pltpu.CompilerParams(collective_id=0, has_side_effects=True,
                                                 vmem_limit_bytes=66_000_000),
        )(lengths, hidden, latent_cache, rope_t, w_uq, wqr_t, w_uk, w_uv, w_out)

    row_spec, cache_spec = P('batch', None), P('batch', ('ctx', 'seq'), None)
    head_spec, proj_spec = P('seq', None, None), P(None, 'seq', None)
    return jax.shard_map(local_step, mesh=mesh,
                         in_specs=(row_spec, P('batch'), cache_spec, cache_spec, proj_spec, proj_spec, head_spec, head_spec, head_spec),
                         out_specs=row_spec, check_vma=False)
```

```python
import functools

import jax
import jax.numpy as jnp
from jax import lax
from jax.experimental import pallas as pl
from jax.experimental.pallas import tpu as pltpu
from jax.sharding import PartitionSpec as P

MESH = pl.DeviceIdType.MESH
F32, BF16 = jnp.float32, jnp.bfloat16
NEG = -3.0e38

ROWS, D, HLOC, NOPE, ROPE, LAT, VAL = 16, 6144, 16, 128, 64, 512, 128
TLOC = 512
QW = LAT + 128
CH = 1536
NCH = D // CH
BLK = CH // 128
QUART = D // 4
PACE = 1.2
AHEAD = 5


def mm(a, b):
    return lax.dot_general(a, b, (((1,), (0,)), ((), ())), preferred_element_type=F32)


def mm_nt(a, b):
    return lax.dot_general(a, b, (((1,), (1,)), ((), ())), preferred_element_type=F32)


def onehot(shape, fn):
    i = lax.broadcasted_iota(jnp.int32, shape, 0)
    j = lax.broadcasted_iota(jnp.int32, shape, 1)
    return jnp.where(fn(i, j), 1.0, 0.0).astype(BF16)


def pack(ms, ls):
    lane = lax.broadcasted_iota(jnp.int32, (8, 128), 1)
    t = jnp.zeros((8, 128), F32)
    for i in range(2):
        for at, v in ((i, ms[i][0:8]), (2 + i, ms[i][8:16]), (4 + i, ls[i][0:8]), (6 + i, ls[i][8:16])):
            t = jnp.where(lane == at, v, t)
    return t


def unpack(t, i):
    return [jnp.concatenate([t[:, at + i:at + i + 1], t[:, at + 2 + i:at + 3 + i]], axis=0) for at in (0, 4)]


def merge(refs):
    out, nm, nl = [], [], []
    tiles = [r[128:136] for r in refs]
    for i in range(2):
        mls = [unpack(t, i) for t in tiles]
        m = functools.reduce(jnp.maximum, [v[0] for v in mls])
        fs = [jnp.exp(v[0] - m) for v in mls]
        nl.append(functools.reduce(jnp.add, [v[1] * f for v, f in zip(mls, fs)]))
        nm.append(m)
        for c in range(4):
            at = 16 * (4 * i + c)
            out.append(functools.reduce(jnp.add, [r[at:at + 16] * f for r, f in zip(refs, fs)]))
    return out, nm, nl


def kernel(len_ref, hid_hbm, cache_hbm, rope_hbm, wuq_hbm, wqr_hbm, wuk_hbm, wuv_hbm, wout_hbm, out_ref,
           hid, cache, rope, wuq, wqr, wuk, wuv, wout, rep, zq, xq, qg, sbuf, acc, racc, yra, zra,
           yb, yr, tr, fin, hsel, outf,
           lsem, usem, csem, q_s, q_r, a_s, a_r, d_s, d_r, y_s, y_r, z_s, z_r, e_s, e_r, t_s, t_r, f_s, f_r):
    x = lax.axis_index("batch")
    z = lax.axis_index("ctx")
    s = lax.axis_index("seq")
    y, k = s // 2, s % 2
    sp = s + 1 - 2 * k
    sy = s + 2 - 4 * y
    spy = sp + 2 - 4 * y
    zx = {1: z + 1 - 2 * (z % 2), 2: z + 2 - 4 * (z // 2), 3: 3 - z}
    inner = ((z + 1) // 2) % 2
    gs = [3 * (1 - z // 2), 2 - z // 2, zx[1], z]

    dev_p, dev_y = (x, z, sp), (x, z, sy)
    dev_z = {j: (x, zx[j], s) for j in zx}
    peers = [dev_p, dev_y, dev_z[1], dev_z[2], dev_z[3]]

    def local(src, dst, sem, priority=1):
        c = pltpu.make_async_copy(src, dst, sem)
        c.start(priority=priority)
        return c

    def remote(src, dst, ss, rs, dev):
        return pltpu.make_async_remote_copy(src_ref=src, dst_ref=dst, send_sem=ss, recv_sem=rs,
                                            device_id=dev, device_id_type=MESH)

    def go(c):
        c.start()

    own4 = pl.ds(pl.multiple_of(4 * z, 4), 4)
    c_hid = local(hid_hbm, hid, lsem.at[0], 0)

    def load_uq(i):
        return local(wuq_hbm.at[pl.ds(i * CH, CH), own4, :], wuq.at[i], usem.at[i])

    c_uq = [load_uq(i) for i in range(NCH)]
    c_qr = local(wqr_hbm.at[own4], wqr, lsem.at[1])

    barrier = pltpu.get_barrier_semaphore()
    for d in peers:
        pl.semaphore_signal(barrier, inc=1, device_id=d, device_id_type=MESH)

    spread = onehot((128, 512), lambda i, j: j // 4 == i)
    lane = lax.broadcasted_iota(jnp.int32, (16, 128), 1)
    masks = [jnp.where(lane % 4 == h, 1.0, 0.0).astype(BF16) for h in range(4)]
    wide = [jnp.concatenate([m] * (CH * 4 // 128), axis=1) for m in masks]
    c_hid.wait()
    for t in range(NCH):
        blk = jnp.concatenate([hid[:, (BLK * t + i) * 128:(BLK * t + i + 1) * 128] for i in range(BLK)], axis=0)
        rep[pl.ds(BLK * t, BLK)] = mm(blk, spread).astype(BF16).reshape(BLK, 16, 512)
    qn = [jnp.zeros((64, NOPE), F32)] * 2
    for i in range(0, NCH, 2):
        c_uq[i].wait()
        c_uq[i + 1].wait()
        for part in range(2):
            for n in range(2):
                at, size = part * (BLK // 2), BLK // 2
                r = jnp.concatenate([rep[(i + n) * BLK + at + t] for t in range(size)], axis=1)
                lhs = jnp.concatenate([r * m[:, :size * 512] for m in wide], axis=0)
                qn[n] = qn[n] + mm(lhs, wuq[i + n, at * 128:(at + size) * 128].reshape(size * 512, NOPE))
        if i == 0:
            c_uk = local(wuk_hbm, wuk, lsem.at[2])
    c_qr.wait()
    qr = jnp.concatenate([mm_nt(hid[...], wqr[2 * h:2 * h + 2].reshape(2 * ROPE, D)) for h in range(2)], axis=1)
    qr = qr.astype(BF16)
    zq[z, 64:80] = qr[:, :128]
    zq[z, 80:96] = qr[:, 128:]
    zq[z, 0:64] = (qn[0] + qn[1]).astype(BF16)
    c_rope = local(rope_hbm, rope, lsem.at[3])
    c_cache = local(cache_hbm, cache, csem.at[0])
    c_uv = local(wuv_hbm, wuv, lsem.at[4])
    c_out = local(wout_hbm, wout, lsem.at[5])

    pl.semaphore_wait(barrier, len(peers))
    def give_z():
        for j in (3, 2, 1):
            remote(zq.at[z], zq.at[z], q_s.at[0], q_r.at[z], dev_z[j]).start()

    give_z()
    pick = onehot((16, 16), lambda i, j: 4 * z + i == j)
    hsel[...] = mm(pick, hid[...])[0:4]

    def row_of(i):
        return sum((jnp.where(i // 4 == n, 4 * g, 0) for n, g in enumerate(gs))) + i % 4

    perm = onehot((256, 256), lambda i, j: (i % 16) * 16 + row_of(i // 16) == j)

    def latent(zz):
        for h in range(4):
            ql = mm(zq[zz, 16 * h:16 * h + 16], wuk[4 * zz + h]).astype(BF16)
            t = zq[zz, 64 + 16 * (h // 2):80 + 16 * (h // 2)]
            if h % 2:
                t = jnp.concatenate([t[:, 64:], t[:, :64]], axis=1)
            xq[4 * zz + h] = jnp.concatenate([ql, t], axis=1)

    c_uk.wait()
    latent(z)
    for j in (1, 2, 3):
        remote(zq.at[zx[j]], zq.at[zx[j]], q_s.at[0], q_r.at[zx[j]], dev_p).wait_recv()
        latent(zx[j])
    qp = mm(perm, xq[...].reshape(256, QW)).astype(BF16)
    def give(u):
        go(remote(qg.at[u, 0], qg.at[u, 1], a_s.at[0], a_r.at[u, 0], dev_y))
        go(remote(qg.at[u, 0], qg.at[u, 2], a_s.at[1], a_r.at[u, 1], dev_p))

    for u in range(8):
        qg[u, 0] = qp[32 * u:32 * u + 32]
        if u < AHEAD:
            give(u)

    def arrived(u, n):
        remote(qg.at[u, n], qg.at[u, n], a_s.at[0], a_r.at[u, n - 1], dev_p).wait_recv()

    def forward(u):
        arrived(u, 1)
        if u + AHEAD < 8:
            give(u + AHEAD)
        go(remote(qg.at[u, 1], qg.at[u, 3], a_s.at[2], a_r.at[u, 2], dev_p))

    scale = (NOPE + ROPE) ** -0.5
    t0 = (z * 4 + s) * TLOC

    def rows_of(u):
        return [4 * gs[u // 2] + 2 * (u % 2) + i for i in range(2)]

    def scores(u):
        for i, b in enumerate(rows_of(u)):
            q = jnp.concatenate([qg[u, p, 16 * i:16 * i + 16, :] for p in range(4)], axis=0)
            sbuf[u % 2, i] = mm_nt(q[:, :LAT], cache[b]) + mm(q[:, LAT:LAT + ROPE], rope[b])

    def attend(u):
        ws, ms, ls = [], [], []
        for i, b in enumerate(rows_of(u)):
            valid = lax.broadcasted_iota(jnp.int32, (64, TLOC), 1) < len_ref[b] - t0
            v = jnp.where(valid, sbuf[u % 2, i] * scale, NEG)
            m = jnp.max(v, axis=1, keepdims=True)
            w = jnp.where(valid, jnp.exp(v - m), 0.0)
            ms.append(m)
            ls.append(jnp.sum(w, axis=1, keepdims=True))
            ws.append(w.astype(BF16))
        for i, b in enumerate(rows_of(u)):
            o = mm(ws[i], cache[b])
            for p in range(4):
                for c in range(4):
                    acc[u, p, 16 * (4 * i + c):16 * (4 * i + c) + 16] = o[16 * p:16 * p + 16, 128 * c:128 * c + 128]
        for p in range(4):
            cut = slice(16 * p, 16 * p + 16)
            acc[u, p, 128:136] = pack([m[cut] for m in ms], [l[cut] for l in ls])

    def d_copy(u):
        return remote(acc.at[u, pl.ds(2, 2)], racc.at[u], d_s.at[0], d_r.at[u], dev_p)

    def y_copy(u):
        return remote(acc.at[u, 1], yra.at[u], y_s.at[0], y_r.at[u], dev_y)

    def z_copy(u):
        n, h = u // 2, u % 2
        to = zx[1] if n == 2 else inner * gs[n] + (1 - inner) * zx[1]
        at = 2 if n == 2 else inner * 3 + (1 - inner) * n
        return remote(acc.at[u, 0], zra.at[at, h], z_s.at[0], z_r.at[at, h], (x, to, s))

    def z_wait(at, h):
        remote(zra.at[at, h], zra.at[at, h], z_s.at[0], z_r.at[at, h], dev_p).wait_recv()

    def add(u, n, other):
        out, m, l = merge([acc[u, n], other])
        for c, o in enumerate(out):
            acc[u, n, 16 * c:16 * c + 16] = o
        acc[u, n, 128:136] = pack(m, l)

    def ready(u):
        arrived(u, 2)
        arrived(u, 3)
        if u < 7:
            forward(u + 1)
        scores(u)

    def stage_r(u):
        ready(u)

    def stage_a(u):
        if 1 < u < 7:
            ready(u + 1)
        attend(u)
        go(d_copy(u))

    def stage_y(u):
        d_copy(u).wait_recv()
        add(u, 1, racc[u, 1])
        go(y_copy(u))
        add(u, 0, racc[u, 0])

    def stage_z(u):
        y_copy(u).wait_recv()
        add(u, 0, yra[u])
        if u < 4:
            @pl.when(inner == 0)
            def _():
                z_copy(u).start()
        elif u < 6:
            go(z_copy(u))

    def stage_c(u):
        @pl.when(inner == 1)
        def _():
            z_wait(u // 2, u % 2)
            add(u, 0, zra[u // 2, u % 2])
            z_copy(u).start()

    forward(0)
    c_rope.wait()
    c_cache.wait()
    plan = [(-1, stage_r, 0), (0.1, stage_r, 1), (0.4, stage_r, 2)]
    first = {(stage_a, 1): 0.2, (stage_y, 0): 0.3, (stage_y, 1): 0.5}
    for u in range(8):
        at = PACE * (u + 5) if u < 4 else 1.47 * u + 4.9
        plan += [(PACE * u, stage_a, u), (PACE * (u + 1) + (0.1 if u else -0.9), stage_y, u), (at, stage_z, u)]
        if u < 4:
            plan.append((at + 3.6, stage_c, u))
    for _, stage, u in sorted(plan, key=lambda e: first.get(e[1:], e[0])):
        stage(u)

    for at in (2, 3):
        for h in range(2):
            z_wait(at, h)
    c_uv.wait()
    c_out.wait()
    ol = []
    for h in range(2):
        u = 6 + h
        out, m, l = merge([acc[u, 0], zra[2, h], zra[3, h]])
        ol += [jnp.concatenate([(out[4 * i + c] / l[i]).astype(BF16) for c in range(4)], axis=1) for i in range(2)]
    ol = jnp.concatenate(ol, axis=0)
    vs = []
    head = lax.broadcasted_iota(jnp.int32, (64, VAL), 0) % 16
    for h in range(HLOC):
        vs.append(jnp.where(head == h, mm(ol, wuv[h]), 0.0).astype(BF16))
    v = jnp.concatenate(vs, axis=1)
    fold = onehot((16, 64), lambda i, j: j // 16 == i)
    v = mm(fold, v).astype(BF16)

    def cols(c):
        return mm(v, wout[:, :, c * QUART:(c + 1) * QUART].reshape(HLOC * VAL, QUART))[0:4]

    def e_copy(c):
        return remote(yb.at[c], yr.at[c % 2], e_s.at[0], e_r.at[c % 2], dev_p)

    def t_copy(n):
        return remote(tr.at[0, n], tr.at[1, n], t_s.at[0], t_r.at[n], dev_y)

    def pair(c):
        n = c % 2
        e_copy(c).wait_recv()
        tr[0, n] = yb[c] + yr[n]
        t_copy(n).start()

    def finish(n):
        t_copy(n).wait_recv()
        c = 2 * k + n
        res = hsel[:, pl.ds(pl.multiple_of(c * QUART, QUART), QUART)] + (tr[0, n] + tr[1, n])
        fin[4 * z + c] = res.astype(BF16)
        for j in (3, 2, 1):
            go(remote(fin.at[4 * z + c], fin.at[4 * z + c], f_s.at[0], f_r.at[n, j], dev_z[j]))
        go(remote(fin.at[4 * z + c], fin.at[4 * z + c], f_s.at[0], f_r.at[n, 0], dev_p))

    for c in range(4):
        yb[c] = cols(c)
        pl.when(k == 1 - c // 2)(lambda: e_copy(c).start())
        if c == 1:
            pl.when(k == 0)(lambda: pair(0))
        elif c == 2:
            pl.when(k == 0)(lambda: pair(1))
        elif c == 3:
            pl.when(k == 1)(lambda: pair(2))
    pl.when(k == 1)(lambda: pair(3))
    for n in range(2):
        finish(n)
    for n in range(2):
        for j in (1, 2, 3):
            at = fin.at[4 * zx[j] + 2 * k + n]
            remote(at, at, f_s.at[0], f_r.at[n, j], dev_p).wait_recv()
            go(remote(at, at, f_s.at[0], f_r.at[n, 3 + j], dev_p))
    for n in range(2):
        for j, zz in enumerate((z, zx[1], zx[2], zx[3])):
            at = fin.at[4 * zz + 2 * (1 - k) + n]
            remote(at, at, f_s.at[0], f_r.at[n, 3 + j if j else 0], dev_p).wait_recv()
    for i in range(4):
        for c in range(4):
            outf[4 * i:4 * i + 4, c * QUART:(c + 1) * QUART] = fin[4 * i + c].astype(F32)
    out_ref[...] = outf[...].astype(BF16)
    for src, sem in ((zq.at[pl.ds(0, 3)], q_s.at[0]), (qg.at[:, 0], a_s.at[0]), (qg.at[:, 0], a_s.at[1]), (qg.at[:, 1], a_s.at[2]),
                     (acc.at[:, pl.ds(2, 2)], d_s.at[0]), (acc.at[:, 1], y_s.at[0]), (acc.at[pl.ds(0, 6), 0], z_s.at[0]),
                     (yb.at[pl.ds(0, 2)], e_s.at[0]), (tr.at[0], t_s.at[0]), (fin.at[pl.ds(0, 14)], f_s.at[0])):
        remote(src, src, sem, d_r.at[0], dev_p).wait_send()


def solution(mesh):
    def local_step(hidden, lengths, latent_cache, rope_keys, w_uq, w_qr, w_uk, w_uv, w_out):
        rope_t = jnp.transpose(rope_keys, (0, 2, 1))
        wqr_t = jnp.transpose(w_qr, (1, 2, 0))
        anyspec = pl.BlockSpec(memory_space=pl.ANY)
        dma = pltpu.SemaphoreType.DMA
        scratch = [
            pltpu.VMEM((ROWS, D), BF16),
            pltpu.VMEM((ROWS, TLOC, LAT), BF16),
            pltpu.VMEM((ROWS, ROPE, TLOC), BF16),
            pltpu.VMEM((NCH, CH, 4, NOPE), BF16),
            pltpu.VMEM((4, ROPE, D), BF16),
            pltpu.VMEM((HLOC, NOPE, LAT), BF16),
            pltpu.VMEM((HLOC, LAT, VAL), BF16),
            pltpu.VMEM((HLOC, VAL, D), BF16),
            pltpu.VMEM((48, 16, 512), BF16),
            pltpu.VMEM((4, 96, 128), BF16),
            pltpu.VMEM((HLOC, 16, QW), BF16),
            pltpu.VMEM((8, 4, 32, QW), BF16),
            pltpu.VMEM((2, 2, 64, TLOC), F32),
            pltpu.VMEM((8, 4, 136, 128), F32),
            pltpu.VMEM((8, 2, 136, 128), F32),
            pltpu.VMEM((8, 136, 128), F32),
            pltpu.VMEM((4, 2, 136, 128), F32),
            pltpu.VMEM((4, 4, QUART), F32),
            pltpu.VMEM((2, 4, QUART), F32),
            pltpu.VMEM((2, 2, 4, QUART), F32),
            pltpu.VMEM((16, 4, QUART), BF16),
            pltpu.VMEM((4, D), F32),
            pltpu.VMEM((ROWS, D), F32),
            dma((6,)), dma((NCH,)), dma((1,)),
            dma((1,)), dma((4,)),
            dma((3,)), dma((8, 3)),
            dma((1,)), dma((8,)),
            dma((1,)), dma((8,)),
            dma((1,)), dma((4, 2)),
            dma((1,)), dma((2,)), dma((1,)), dma((2,)),
            dma((1,)), dma((2, 7)),
        ]
        return pl.pallas_call(
            kernel,
            out_shape=pltpu.VMEM((ROWS, D), BF16),
            in_specs=[pl.BlockSpec(memory_space=pltpu.SMEM)] + [anyspec] * 8,
            out_specs=pl.BlockSpec(memory_space=pltpu.VMEM),
            scratch_shapes=scratch,
            compiler_params=pltpu.CompilerParams(collective_id=0, has_side_effects=True,
                                                 vmem_limit_bytes=66_000_000),
        )(lengths, hidden, latent_cache, rope_t, w_uq, wqr_t, w_uk, w_uv, w_out)

    row_spec, cache_spec = P('batch', None), P('batch', ('ctx', 'seq'), None)
    head_spec, proj_spec = P('seq', None, None), P(None, 'seq', None)
    return jax.shard_map(local_step, mesh=mesh,
                         in_specs=(row_spec, P('batch'), cache_spec, cache_spec, proj_spec, proj_spec, head_spec, head_spec, head_spec),
                         out_specs=row_spec, check_vma=False)
```

```python
import functools

import jax
import jax.numpy as jnp
from jax import lax
from jax.experimental import pallas as pl
from jax.experimental.pallas import tpu as pltpu
from jax.sharding import PartitionSpec as P

MESH = pl.DeviceIdType.MESH
F32, BF16 = jnp.float32, jnp.bfloat16
NEG = -3.0e38

ROWS, D, HLOC, NOPE, ROPE, LAT, VAL = 16, 6144, 16, 128, 64, 512, 128
TLOC = 512
QW = LAT + 128
CH = 1536
NCH = D // CH
BLK = CH // 128
QUART = D // 4
PACE = 1.2
LAG = 3.6
AHEAD = 5


def mm(a, b):
    return lax.dot_general(a, b, (((1,), (0,)), ((), ())), preferred_element_type=F32)


def mm_nt(a, b):
    return lax.dot_general(a, b, (((1,), (1,)), ((), ())), preferred_element_type=F32)


def onehot(shape, fn):
    i = lax.broadcasted_iota(jnp.int32, shape, 0)
    j = lax.broadcasted_iota(jnp.int32, shape, 1)
    return jnp.where(fn(i, j), 1.0, 0.0).astype(BF16)


def pack(ms, ls):
    lane = lax.broadcasted_iota(jnp.int32, (8, 128), 1)
    t = jnp.zeros((8, 128), F32)
    for i in range(2):
        for at, v in ((i, ms[i][0:8]), (2 + i, ms[i][8:16]), (4 + i, ls[i][0:8]), (6 + i, ls[i][8:16])):
            t = jnp.where(lane == at, v, t)
    return t


def unpack(t, i):
    return [jnp.concatenate([t[:, at + i:at + i + 1], t[:, at + 2 + i:at + 3 + i]], axis=0) for at in (0, 4)]


def merge(refs):
    out, nm, nl = [], [], []
    tiles = [r[128:136] for r in refs]
    for i in range(2):
        mls = [unpack(t, i) for t in tiles]
        m = functools.reduce(jnp.maximum, [v[0] for v in mls])
        fs = [jnp.exp(v[0] - m) for v in mls]
        nl.append(functools.reduce(jnp.add, [v[1] * f for v, f in zip(mls, fs)]))
        nm.append(m)
        for c in range(4):
            at = 16 * (4 * i + c)
            out.append(functools.reduce(jnp.add, [r[at:at + 16] * f for r, f in zip(refs, fs)]))
    return out, nm, nl


def kernel(len_ref, hid_hbm, cache_hbm, rope_hbm, wuq_hbm, wqr_hbm, wuk_hbm, wuv_hbm, wout_hbm, out_ref,
           hid, cache, rope, wuq, wqr, wuk, wuv, wout, rep, zq, xq, qg, sbuf, acc, racc, yra, zra,
           yb, yr, tr, fin, hsel, outf,
           lsem, usem, csem, q_s, q_r, a_s, a_r, d_s, d_r, y_s, y_r, z_s, z_r, e_s, e_r, t_s, t_r, f_s, f_r):
    x = lax.axis_index("batch")
    z = lax.axis_index("ctx")
    s = lax.axis_index("seq")
    y, k = s // 2, s % 2
    sp = s + 1 - 2 * k
    sy = s + 2 - 4 * y
    spy = sp + 2 - 4 * y
    zx = {1: z + 1 - 2 * (z % 2), 2: z + 2 - 4 * (z // 2), 3: 3 - z}
    inner = ((z + 1) // 2) % 2
    gs = [3 * (1 - z // 2), 2 - z // 2, zx[1], z]

    dev_p, dev_y = (x, z, sp), (x, z, sy)
    dev_z = {j: (x, zx[j], s) for j in zx}
    peers = [dev_p, dev_y, dev_z[1], dev_z[2], dev_z[3]]

    def local(src, dst, sem, priority=1):
        c = pltpu.make_async_copy(src, dst, sem)
        c.start(priority=priority)
        return c

    def remote(src, dst, ss, rs, dev):
        return pltpu.make_async_remote_copy(src_ref=src, dst_ref=dst, send_sem=ss, recv_sem=rs,
                                            device_id=dev, device_id_type=MESH)

    def go(c):
        c.start()

    own4 = pl.ds(pl.multiple_of(4 * z, 4), 4)
    c_hid = local(hid_hbm, hid, lsem.at[0], 0)

    def load_uq(i):
        return local(wuq_hbm.at[pl.ds(i * 2 * CH, 2 * CH), own4, :], wuq.at[i], usem.at[i])

    c_uq = [load_uq(i) for i in range(NCH // 2)]
    c_qr = local(wqr_hbm.at[own4], wqr, lsem.at[1])

    barrier = pltpu.get_barrier_semaphore()
    for d in peers:
        pl.semaphore_signal(barrier, inc=1, device_id=d, device_id_type=MESH)

    spread = onehot((128, 512), lambda i, j: j // 4 == i)
    lane = lax.broadcasted_iota(jnp.int32, (16, 128), 1)
    masks = [jnp.where(lane % 4 == h, 1.0, 0.0).astype(BF16) for h in range(4)]
    wide = [jnp.concatenate([m] * (CH * 4 // 128), axis=1) for m in masks]
    c_hid.wait()
    for t in range(NCH):
        blk = jnp.concatenate([hid[:, (BLK * t + i) * 128:(BLK * t + i + 1) * 128] for i in range(BLK)], axis=0)
        rep[pl.ds(BLK * t, BLK)] = mm(blk, spread).astype(BF16).reshape(BLK, 16, 512)
    qn = [jnp.zeros((64, NOPE), F32)] * 2
    for i in range(0, NCH, 2):
        c_uq[i // 2].wait()
        for part in range(2):
            for n in range(2):
                at, size = part * (BLK // 2), BLK // 2
                r = jnp.concatenate([rep[(i + n) * BLK + at + t] for t in range(size)], axis=1)
                lhs = jnp.concatenate([r * m[:, :size * 512] for m in wide], axis=0)
                qn[n] = qn[n] + mm(lhs, wuq[i // 2, (n * BLK + at) * 128:(n * BLK + at + size) * 128].reshape(size * 512, NOPE))
        if i == 0:
            c_uk = local(wuk_hbm, wuk, lsem.at[2])
    c_qr.wait()
    qr = jnp.concatenate([mm_nt(hid[...], wqr[2 * h:2 * h + 2].reshape(2 * ROPE, D)) for h in range(2)], axis=1)
    qr = qr.astype(BF16)
    zq[z, 64:80] = qr[:, :128]
    zq[z, 80:96] = qr[:, 128:]
    zq[z, 0:64] = (qn[0] + qn[1]).astype(BF16)
    c_rope = local(rope_hbm, rope, lsem.at[3])
    c_cache = local(cache_hbm, cache, csem)
    c_uv = local(wuv_hbm, wuv, lsem.at[4])
    c_out = local(wout_hbm, wout, lsem.at[5])

    pl.semaphore_wait(barrier, len(peers))
    def give_z():
        for j in (3, 2, 1):
            remote(zq.at[z], zq.at[z], q_s, q_r.at[z], dev_z[j]).start()

    give_z()
    pick = onehot((16, 16), lambda i, j: 4 * z + i == j)
    hsel[...] = mm(pick, hid[...])[0:4]

    def row_of(i):
        return sum((jnp.where(i // 4 == n, 4 * g, 0) for n, g in enumerate(gs))) + i % 4

    perm = onehot((256, 256), lambda i, j: (i % 16) * 16 + row_of(i // 16) == j)

    def latent(zz):
        for h in range(4):
            ql = mm(zq[zz, 16 * h:16 * h + 16], wuk[4 * zz + h]).astype(BF16)
            t = zq[zz, 64 + 16 * (h // 2):80 + 16 * (h // 2)]
            if h % 2:
                t = jnp.concatenate([t[:, 64:], t[:, :64]], axis=1)
            xq[4 * zz + h] = jnp.concatenate([ql, t], axis=1)

    c_uk.wait()
    latent(z)
    for j in (1, 2, 3):
        remote(zq.at[zx[j]], zq.at[zx[j]], q_s, q_r.at[zx[j]], dev_p).wait_recv()
        latent(zx[j])
    qp = mm(perm, xq[...].reshape(256, QW)).astype(BF16)
    def give(u):
        go(remote(qg.at[u, 0], qg.at[u, 1], a_s.at[0], a_r.at[u, 0], dev_y))
        go(remote(qg.at[u, 0], qg.at[u, 2], a_s.at[1], a_r.at[u, 1], dev_p))

    for u in range(8):
        qg[u, 0] = qp[32 * u:32 * u + 32]
        if u < AHEAD:
            give(u)

    def arrived(u, n):
        remote(qg.at[u, n], qg.at[u, n], a_s.at[0], a_r.at[u, n - 1], dev_p).wait_recv()

    def forward(u):
        arrived(u, 1)
        if u + AHEAD < 8:
            give(u + AHEAD)
        go(remote(qg.at[u, 1], qg.at[u, 3], a_s.at[2], a_r.at[u, 2], dev_p))

    scale = (NOPE + ROPE) ** -0.5
    t0 = (z * 4 + s) * TLOC

    def rows_of(u):
        return [4 * gs[u // 2] + 2 * (u % 2) + i for i in range(2)]

    def scores(u):
        for i, b in enumerate(rows_of(u)):
            q = jnp.concatenate([qg[u, p, 16 * i:16 * i + 16, :] for p in range(4)], axis=0)
            sbuf[u % 2, i] = mm_nt(q[:, :LAT], cache[b]) + mm(q[:, LAT:LAT + ROPE], rope[b])

    def attend(u):
        ws, ms, ls = [], [], []
        for i, b in enumerate(rows_of(u)):
            valid = lax.broadcasted_iota(jnp.int32, (64, TLOC), 1) < len_ref[b] - t0
            v = jnp.where(valid, sbuf[u % 2, i] * scale, NEG)
            m = jnp.max(v, axis=1, keepdims=True)
            w = jnp.where(valid, jnp.exp(v - m), 0.0)
            ms.append(m)
            ls.append(jnp.sum(w, axis=1, keepdims=True))
            ws.append(w.astype(BF16))
        for i, b in enumerate(rows_of(u)):
            o = mm(ws[i], cache[b])
            for p in range(4):
                for c in range(4):
                    acc[u, p, 16 * (4 * i + c):16 * (4 * i + c) + 16] = o[16 * p:16 * p + 16, 128 * c:128 * c + 128]
        for p in range(4):
            cut = slice(16 * p, 16 * p + 16)
            acc[u, p, 128:136] = pack([m[cut] for m in ms], [l[cut] for l in ls])

    def d_copy(u):
        return remote(acc.at[u, pl.ds(2, 2)], racc.at[u], d_s, d_r.at[u], dev_p)

    def y_copy(u):
        return remote(acc.at[u, 1], yra.at[u], y_s, y_r.at[u], dev_y)

    def z_copy(u):
        n, h = u // 2, u % 2
        to = zx[1] if n == 2 else inner * gs[n] + (1 - inner) * zx[1]
        at = 2 if n == 2 else inner * 3 + (1 - inner) * n
        return remote(acc.at[u, 0], zra.at[at, h], z_s, z_r.at[at, h], (x, to, s))

    def z_wait(at, h):
        remote(zra.at[at, h], zra.at[at, h], z_s, z_r.at[at, h], dev_p).wait_recv()

    def add(u, n, other):
        out, m, l = merge([acc[u, n], other])
        for c, o in enumerate(out):
            acc[u, n, 16 * c:16 * c + 16] = o
        acc[u, n, 128:136] = pack(m, l)

    def ready(u):
        arrived(u, 2)
        arrived(u, 3)
        if u < 7:
            forward(u + 1)
        scores(u)

    def stage_r(u):
        ready(u)

    def stage_a(u):
        if 1 < u < 7:
            ready(u + 1)
        attend(u)
        go(d_copy(u))

    def stage_y(u):
        d_copy(u).wait_recv()
        add(u, 1, racc[u, 1])
        go(y_copy(u))
        add(u, 0, racc[u, 0])

    def stage_z(u):
        y_copy(u).wait_recv()
        add(u, 0, yra[u])
        if u < 4:
            @pl.when(inner == 0)
            def _():
                z_copy(u).start()
        elif u < 6:
            go(z_copy(u))

    def stage_c(u):
        @pl.when(inner == 1)
        def _():
            z_wait(u // 2, u % 2)
            add(u, 0, zra[u // 2, u % 2])
            z_copy(u).start()

    forward(0)
    c_rope.wait()
    c_cache.wait()
    plan = [(-1, stage_r, 0), (0.1, stage_r, 1), (0.4, stage_r, 2)]
    first = {(stage_a, 1): 0.2, (stage_y, 0): 0.3, (stage_y, 1): 0.5}
    for u in range(8):
        at = PACE * (u + 5) if u < 4 else 1.47 * u + 3.9
        plan += [(PACE * u, stage_a, u), (PACE * (u + 1) + (0.1 if u else -0.9), stage_y, u), (at, stage_z, u)]
        if u < 4:
            plan.append((at + LAG, stage_c, u))
    for _, stage, u in sorted(plan, key=lambda e: first.get(e[1:], e[0])):
        stage(u)

    c_uv.wait()
    c_out.wait()
    ol = []
    for h in range(2):
        u = 6 + h
        z_wait(2, h)
        z_wait(3, h)
        if h:
            pass
        out, m, l = merge([acc[u, 0], zra[2, h], zra[3, h]])
        ol += [jnp.concatenate([(out[4 * i + c] / l[i]).astype(BF16) for c in range(4)], axis=1) for i in range(2)]
    ol = jnp.concatenate(ol, axis=0)
    vs = []
    head = lax.broadcasted_iota(jnp.int32, (64, VAL), 0) % 16
    for h in range(HLOC):
        vs.append(jnp.where(head == h, mm(ol, wuv[h]), 0.0).astype(BF16))
    v = jnp.concatenate(vs, axis=1)
    fold = onehot((16, 64), lambda i, j: j // 16 == i)
    v = mm(fold, v).astype(BF16)

    def cols(c):
        return mm(v, wout[:, :, c * QUART:(c + 1) * QUART].reshape(HLOC * VAL, QUART))[0:4]

    def e_copy(c):
        return remote(yb.at[c], yr.at[c % 2], e_s, e_r.at[c % 2], dev_p)

    def t_copy(n):
        return remote(tr.at[0, n], tr.at[1, n], t_s, t_r.at[n], dev_y)

    def pair(c):
        n = c % 2
        e_copy(c).wait_recv()
        tr[0, n] = yb[c] + yr[n]
        t_copy(n).start()

    def finish(n):
        t_copy(n).wait_recv()
        c = 2 * k + n
        res = hsel[:, pl.ds(pl.multiple_of(c * QUART, QUART), QUART)] + (tr[0, n] + tr[1, n])
        fin[4 * z + c] = res.astype(BF16)
        for j in (3, 2, 1):
            go(remote(fin.at[4 * z + c], fin.at[4 * z + c], f_s, f_r.at[n, j], dev_z[j]))
        go(remote(fin.at[4 * z + c], fin.at[4 * z + c], f_s, f_r.at[n, 0], dev_p))

    for c in range(4):
        yb[c] = cols(c)
        pl.when(k == 1 - c // 2)(lambda: e_copy(c).start())
        if c == 1:
            pl.when(k == 0)(lambda: pair(0))
        elif c == 2:
            pl.when(k == 0)(lambda: pair(1))
        elif c == 3:
            pl.when(k == 1)(lambda: pair(2))
    pl.when(k == 1)(lambda: pair(3))
    for n in range(2):
        finish(n)
    for n in range(2):
        for j in (1, 2, 3):
            at = fin.at[4 * zx[j] + 2 * k + n]
            remote(at, at, f_s, f_r.at[n, j], dev_p).wait_recv()
            go(remote(at, at, f_s, f_r.at[n, 3 + j], dev_p))
    for n in range(2):
        for j, zz in enumerate((z, zx[1], zx[2], zx[3])):
            at = fin.at[4 * zz + 2 * (1 - k) + n]
            remote(at, at, f_s, f_r.at[n, 3 + j if j else 0], dev_p).wait_recv()
    for i in range(4):
        for c in range(4):
            outf[4 * i:4 * i + 4, c * QUART:(c + 1) * QUART] = fin[4 * i + c].astype(F32)
    out_ref[...] = outf[...].astype(BF16)
    for src, sem in ((zq.at[pl.ds(0, 3)], q_s), (qg.at[:, 0], a_s.at[0]), (qg.at[:, 0], a_s.at[1]), (qg.at[:, 1], a_s.at[2]),
                     (acc.at[:, pl.ds(2, 2)], d_s), (acc.at[:, 1], y_s), (acc.at[pl.ds(0, 6), 0], z_s),
                     (yb.at[pl.ds(0, 2)], e_s), (tr.at[0], t_s), (fin.at[pl.ds(0, 14)], f_s)):
        remote(src, src, sem, d_r.at[0], dev_p).wait_send()


def solution(mesh):
    def local_step(hidden, lengths, latent_cache, rope_keys, w_uq, w_qr, w_uk, w_uv, w_out):
        rope_t = jnp.transpose(rope_keys, (0, 2, 1))
        wqr_t = jnp.transpose(w_qr, (1, 2, 0))
        anyspec = pl.BlockSpec(memory_space=pl.ANY)
        dma = pltpu.SemaphoreType.DMA
        scratch = [
            pltpu.VMEM((ROWS, D), BF16),
            pltpu.VMEM((ROWS, TLOC, LAT), BF16),
            pltpu.VMEM((ROWS, ROPE, TLOC), BF16),
            pltpu.VMEM((NCH // 2, 2 * CH, 4, NOPE), BF16),
            pltpu.VMEM((4, ROPE, D), BF16),
            pltpu.VMEM((HLOC, NOPE, LAT), BF16),
            pltpu.VMEM((HLOC, LAT, VAL), BF16),
            pltpu.VMEM((HLOC, VAL, D), BF16),
            pltpu.VMEM((48, 16, 512), BF16),
            pltpu.VMEM((4, 96, 128), BF16),
            pltpu.VMEM((HLOC, 16, QW), BF16),
            pltpu.VMEM((8, 4, 32, QW), BF16),
            pltpu.VMEM((2, 2, 64, TLOC), F32),
            pltpu.VMEM((8, 4, 136, 128), F32),
            pltpu.VMEM((8, 2, 136, 128), F32),
            pltpu.VMEM((8, 136, 128), F32),
            pltpu.VMEM((4, 2, 136, 128), F32),
            pltpu.VMEM((4, 4, QUART), F32),
            pltpu.VMEM((2, 4, QUART), F32),
            pltpu.VMEM((2, 2, 4, QUART), F32),
            pltpu.VMEM((16, 4, QUART), BF16),
            pltpu.VMEM((4, D), F32),
            pltpu.VMEM((ROWS, D), F32),
            dma((6,)), dma((2,)), dma,
            dma, dma((4,)),
            dma((3,)), dma((8, 3)),
            dma, dma((8,)),
            dma, dma((8,)),
            dma, dma((4, 2)),
            dma, dma((2,)), dma, dma((2,)),
            dma, dma((2, 7)),
        ]
        return pl.pallas_call(
            kernel,
            out_shape=pltpu.VMEM((ROWS, D), BF16),
            in_specs=[pl.BlockSpec(memory_space=pltpu.SMEM)] + [anyspec] * 8,
            out_specs=pl.BlockSpec(memory_space=pltpu.VMEM),
            scratch_shapes=scratch,
            compiler_params=pltpu.CompilerParams(collective_id=0, has_side_effects=True,
                                                 vmem_limit_bytes=66_000_000),
        )(lengths, hidden, latent_cache, rope_t, w_uq, wqr_t, w_uk, w_uv, w_out)

    row_spec, cache_spec = P('batch', None), P('batch', ('ctx', 'seq'), None)
    head_spec, proj_spec = P('seq', None, None), P(None, 'seq', None)
    return jax.shard_map(local_step, mesh=mesh,
                         in_specs=(row_spec, P('batch'), cache_spec, cache_spec, proj_spec, proj_spec, head_spec, head_spec, head_spec),
                         out_specs=row_spec, check_vma=False)
```

```python
import functools

import jax
import jax.numpy as jnp
from jax import lax
from jax.experimental import pallas as pl
from jax.experimental.pallas import tpu as pltpu
from jax.sharding import PartitionSpec as P

MESH = pl.DeviceIdType.MESH
F32, BF16 = jnp.float32, jnp.bfloat16
NEG = -3.0e38

ROWS, D, HLOC, NOPE, ROPE, LAT, VAL = 16, 6144, 16, 128, 64, 512, 128
TLOC = 512
QW = LAT + 128
CH = 1536
NCH = D // CH
BLK = CH // 128
QUART = D // 4
PAIR = 2
PACE = 1.2
LAG = 3.6
AHEAD = 5


def mm(a, b):
    return lax.dot_general(a, b, (((1,), (0,)), ((), ())), preferred_element_type=F32)


def mm_nt(a, b):
    return lax.dot_general(a, b, (((1,), (1,)), ((), ())), preferred_element_type=F32)


def onehot(shape, fn):
    i = lax.broadcasted_iota(jnp.int32, shape, 0)
    j = lax.broadcasted_iota(jnp.int32, shape, 1)
    return jnp.where(fn(i, j), 1.0, 0.0).astype(BF16)


def pack(ms, ls):
    lane = lax.broadcasted_iota(jnp.int32, (8, 128), 1)
    t = jnp.zeros((8, 128), F32)
    for i in range(2):
        for at, v in ((i, ms[i][0:8]), (2 + i, ms[i][8:16]), (4 + i, ls[i][0:8]), (6 + i, ls[i][8:16])):
            t = jnp.where(lane == at, v, t)
    return t


def unpack(t, i):
    return [jnp.concatenate([t[:, at + i:at + i + 1], t[:, at + 2 + i:at + 3 + i]], axis=0) for at in (0, 4)]


def merge(refs):
    out, nm, nl = [], [], []
    tiles = [r[128:136] for r in refs]
    for i in range(2):
        mls = [unpack(t, i) for t in tiles]
        m = functools.reduce(jnp.maximum, [v[0] for v in mls])
        fs = [jnp.exp(v[0] - m) for v in mls]
        nl.append(functools.reduce(jnp.add, [v[1] * f for v, f in zip(mls, fs)]))
        nm.append(m)
        for c in range(4):
            at = 16 * (4 * i + c)
            out.append(functools.reduce(jnp.add, [r[at:at + 16] * f for r, f in zip(refs, fs)]))
    return out, nm, nl


def kernel(len_ref, hid_hbm, cache_hbm, rope_hbm, wuq_hbm, wqr_hbm, wuk_hbm, wuv_hbm, wout_hbm, out_ref,
           hid, cache, rope, wuq, wqr, wuk, wuv, wout, rep, zq, xq, qg, sbuf, acc, racc, yra, zra,
           yb, yr, tr, fin, hsel, outf,
           lsem, usem, csem, q_s, q_r, a_s, a_r, d_s, d_r, y_s, y_r, z_s, z_r, e_s, e_r, t_s, t_r, f_s, f_r):
    x = lax.axis_index("batch")
    z = lax.axis_index("ctx")
    s = lax.axis_index("seq")
    y, k = s // 2, s % 2
    sp = s + 1 - 2 * k
    sy = s + 2 - 4 * y
    spy = sp + 2 - 4 * y
    zx = {1: z + 1 - 2 * (z % 2), 2: z + 2 - 4 * (z // 2), 3: 3 - z}
    inner = ((z + 1) // 2) % 2
    far = [3 * (1 - z // 2), 2 - z // 2]
    outer = 1 - inner
    gs = [inner * zx[1] + outer * far[0], inner * far[0] + outer * far[1], inner * far[1] + outer * zx[1], z]

    dev_p, dev_y = (x, z, sp), (x, z, sy)
    dev_z = {j: (x, zx[j], s) for j in zx}
    peers = [dev_p, dev_y, dev_z[1], dev_z[2], dev_z[3]]

    def local(src, dst, sem, priority=1):
        c = pltpu.make_async_copy(src, dst, sem)
        c.start(priority=priority)
        return c

    def remote(src, dst, ss, rs, dev):
        return pltpu.make_async_remote_copy(src_ref=src, dst_ref=dst, send_sem=ss, recv_sem=rs,
                                            device_id=dev, device_id_type=MESH)

    def go(c):
        c.start()

    own4 = pl.ds(pl.multiple_of(4 * z, 4), 4)
    c_hid = local(hid_hbm, hid, lsem.at[0], 0)

    def load_uq(i):
        return local(wuq_hbm.at[pl.ds(i * 2 * CH, 2 * CH), own4, :], wuq.at[i], usem.at[i])

    c_uq = [load_uq(i) for i in range(NCH // 2)]
    c_qr = local(wqr_hbm.at[own4], wqr, lsem.at[1])

    barrier = pltpu.get_barrier_semaphore()
    for d in peers:
        pl.semaphore_signal(barrier, inc=1, device_id=d, device_id_type=MESH)

    spread = onehot((128, 512), lambda i, j: j // 4 == i)
    lane = lax.broadcasted_iota(jnp.int32, (16, 128), 1)
    masks = [jnp.where(lane % 4 == h, 1.0, 0.0).astype(BF16) for h in range(4)]
    wide = [jnp.concatenate([m] * (CH * 4 // 128), axis=1) for m in masks]
    c_hid.wait()
    for t in range(NCH):
        blk = jnp.concatenate([hid[:, (BLK * t + i) * 128:(BLK * t + i + 1) * 128] for i in range(BLK)], axis=0)
        rep[pl.ds(BLK * t, BLK)] = mm(blk, spread).astype(BF16).reshape(BLK, 16, 512)
    qn = [jnp.zeros((64, NOPE), F32)] * 2
    for i in range(0, NCH, 2):
        c_uq[i // 2].wait()
        for part in range(2):
            for n in range(2):
                at, size = part * (BLK // 2), BLK // 2
                r = jnp.concatenate([rep[(i + n) * BLK + at + t] for t in range(size)], axis=1)
                lhs = jnp.concatenate([r * m[:, :size * 512] for m in wide], axis=0)
                qn[n] = qn[n] + mm(lhs, wuq[i // 2, (n * BLK + at) * 128:(n * BLK + at + size) * 128].reshape(size * 512, NOPE))
        if i == 0:
            c_uk = local(wuk_hbm, wuk, lsem.at[2])
    c_qr.wait()
    qr = jnp.concatenate([mm_nt(hid[...], wqr[2 * h:2 * h + 2].reshape(2 * ROPE, D)) for h in range(2)], axis=1)
    qr = qr.astype(BF16)
    zq[z, 64:80] = qr[:, :128]
    zq[z, 80:96] = qr[:, 128:]
    zq[z, 0:64] = (qn[0] + qn[1]).astype(BF16)
    c_rope = local(rope_hbm, rope, lsem.at[3])
    c_cache = local(cache_hbm, cache, csem)
    c_uv = local(wuv_hbm, wuv, lsem.at[4])
    c_out = local(wout_hbm, wout, lsem.at[5])

    pl.semaphore_wait(barrier, len(peers))
    def give_z():
        for j in (3, 2, 1):
            remote(zq.at[z], zq.at[z], q_s, q_r.at[z], dev_z[j]).start()

    give_z()
    pick = onehot((16, 16), lambda i, j: 4 * z + i == j)
    hsel[...] = mm(pick, hid[...])[0:4]

    def row_of(i):
        return sum((jnp.where(i // 4 == n, 4 * g, 0) for n, g in enumerate(gs))) + i % 4

    perm = onehot((256, 256), lambda i, j: (i % 16) * 16 + row_of(i // 16) == j)

    def latent(zz):
        for h in range(4):
            ql = mm(zq[zz, 16 * h:16 * h + 16], wuk[4 * zz + h]).astype(BF16)
            t = zq[zz, 64 + 16 * (h // 2):80 + 16 * (h // 2)]
            if h % 2:
                t = jnp.concatenate([t[:, 64:], t[:, :64]], axis=1)
            xq[4 * zz + h] = jnp.concatenate([ql, t], axis=1)

    c_uk.wait()
    latent(z)
    for j in (1, 2, 3):
        remote(zq.at[zx[j]], zq.at[zx[j]], q_s, q_r.at[zx[j]], dev_p).wait_recv()
        latent(zx[j])
    qp = mm(perm, xq[...].reshape(256, QW)).astype(BF16)
    def give(u):
        go(remote(qg.at[u, 0], qg.at[u, 1], a_s.at[0], a_r.at[u, 0], dev_y))
        go(remote(qg.at[u, 0], qg.at[u, 2], a_s.at[1], a_r.at[u, 1], dev_p))

    for u in range(8):
        rows = qp[32 * u:32 * u + 32]
        for c in range(4):
            qg[u, 0, 32 * c:32 * c + 32] = rows[:, NOPE * c:NOPE * c + NOPE]
        qg[u, 0, NOPE:] = jnp.concatenate([rows[:16, LAT:LAT + ROPE], rows[16:, LAT:LAT + ROPE]], axis=1)
        if u < AHEAD:
            give(u)

    def arrived(u, n):
        remote(qg.at[u, n], qg.at[u, n], a_s.at[0], a_r.at[u, n - 1], dev_p).wait_recv()

    def forward(u):
        arrived(u, 1)
        if u + AHEAD < 8:
            give(u + AHEAD)
        go(remote(qg.at[u, 1], qg.at[u, 3], a_s.at[2], a_r.at[u, 2], dev_p))

    scale = (NOPE + ROPE) ** -0.5
    t0 = (z * 4 + s) * TLOC

    def rows_of(u):
        return [4 * gs[u // PAIR] + 2 * (u % PAIR) + i for i in range(2)]

    def scores(u):
        for i, b in enumerate(rows_of(u)):
            q = [jnp.concatenate([qg[u, p, 32 * c + 16 * i:32 * c + 16 * i + 16] for p in range(4)], axis=0) for c in range(4)]
            r = jnp.concatenate([qg[u, p, NOPE:] for p in range(4)], axis=0)[:, ROPE * i:ROPE * i + ROPE]
            sbuf[u % PAIR, i] = mm_nt(jnp.concatenate(q, axis=1), cache[b]) + mm(r, rope[b])

    def attend(u):
        ws, ms, ls = [], [], []
        for i, b in enumerate(rows_of(u)):
            valid = lax.broadcasted_iota(jnp.int32, (64, TLOC), 1) < len_ref[b] - t0
            v = jnp.where(valid, sbuf[u % PAIR, i] * scale, NEG)
            m = jnp.max(v, axis=1, keepdims=True)
            w = jnp.where(valid, jnp.exp(v - m), 0.0)
            ms.append(m)
            ls.append(jnp.sum(w, axis=1, keepdims=True))
            ws.append(w.astype(BF16))
        for i, b in enumerate(rows_of(u)):
            o = mm(ws[i], cache[b])
            for p in range(4):
                for c in range(4):
                    acc[u, p, 16 * (4 * i + c):16 * (4 * i + c) + 16] = o[16 * p:16 * p + 16, 128 * c:128 * c + 128]
        for p in range(4):
            cut = slice(16 * p, 16 * p + 16)
            acc[u, p, 128:136] = pack([m[cut] for m in ms], [l[cut] for l in ls])

    def d_copy(u):
        return remote(acc.at[u, pl.ds(2, 2)], racc.at[u], d_s, d_r.at[u], dev_p)

    def y_copy(u):
        return remote(acc.at[u, 1], yra.at[u], y_s, y_r.at[u], dev_y)

    def z_copy(u):
        n, h = u // PAIR, u % PAIR
        to = inner * gs[n] + outer * zx[1]
        at = inner * (3 if n else 2) + outer * n
        return remote(acc.at[u, 0], zra.at[at, h], z_s, z_r.at[at, h], (x, to, s))

    def z_wait(at, h):
        remote(zra.at[at, h], zra.at[at, h], z_s, z_r.at[at, h], dev_p).wait_recv()

    def add(u, n, other):
        out, m, l = merge([acc[u, n], other])
        for c, o in enumerate(out):
            acc[u, n, 16 * c:16 * c + 16] = o
        acc[u, n, 128:136] = pack(m, l)

    def ready(u):
        arrived(u, 2)
        arrived(u, 3)
        if u < 7:
            forward(u + 1)
        scores(u)

    def stage_r(u):
        ready(u)

    def stage_a(u):
        if 1 < u < 7:
            ready(u + 1)
        attend(u)
        go(d_copy(u))

    def stage_y(u):
        d_copy(u).wait_recv()
        add(u, 1, racc[u, 1])
        go(y_copy(u))
        add(u, 0, racc[u, 0])

    def stage_z(u):
        y_copy(u).wait_recv()
        add(u, 0, yra[u])
        if u < 2:
            go(z_copy(u))
        elif u < 6:
            pl.when(inner == 0)(lambda: z_copy(u).start())

    def stage_c(u):
        @pl.when(inner == 1)
        def _():
            z_wait(u // PAIR - 1, u % PAIR)
            add(u, 0, zra[u // PAIR - 1, u % PAIR])
            z_copy(u).start()

    forward(0)
    c_rope.wait()
    c_cache.wait()
    plan = [(-1, stage_r, 0), (0.1, stage_r, 1), (0.4, stage_r, 2)]
    first = {(stage_a, 1): 0.2, (stage_y, 0): 0.3, (stage_y, 1): 0.5}
    for u in range(8):
        at = PACE * (u + 5) if u < 4 else 1.47 * u + 3.9
        plan += [(PACE * u, stage_a, u), (PACE * (u + 1) + (0.1 if u else -0.9), stage_y, u), (at, stage_z, u)]
        if u < 4:
            plan.append((at + LAG, stage_c, u + 2))
    for _, stage, u in sorted(plan, key=lambda e: first.get(e[1:], e[0])):
        stage(u)

    c_uv.wait()
    c_out.wait()
    ol = []
    for h in range(2):
        u = 6 + h
        z_wait(2, h)
        z_wait(3, h)
        if h:
            pass
        out, m, l = merge([acc[u, 0], zra[2, h], zra[3, h]])
        ol += [jnp.concatenate([(out[4 * i + c] / l[i]).astype(BF16) for c in range(4)], axis=1) for i in range(2)]
    ol = jnp.concatenate(ol, axis=0)
    vs = []
    head = lax.broadcasted_iota(jnp.int32, (64, VAL), 0) % 16
    for h in range(HLOC):
        vs.append(jnp.where(head == h, mm(ol, wuv[h]), 0.0).astype(BF16))
    v = jnp.concatenate(vs, axis=1)
    fold = onehot((16, 64), lambda i, j: j // 16 == i)
    v = mm(fold, v).astype(BF16)

    def cols(c):
        return mm(v, wout[:, :, c * QUART:(c + 1) * QUART].reshape(HLOC * VAL, QUART))[0:4]

    def e_copy(c):
        return remote(yb.at[c], yr.at[c % 2], e_s, e_r.at[c % 2], dev_p)

    def t_copy(n):
        return remote(tr.at[0, n], tr.at[1, n], t_s, t_r.at[n], dev_y)

    def pair(c):
        n = c % 2
        e_copy(c).wait_recv()
        tr[0, n] = yb[c] + yr[n]
        t_copy(n).start()

    def finish(n):
        t_copy(n).wait_recv()
        c = 2 * k + n
        res = hsel[:, pl.ds(pl.multiple_of(c * QUART, QUART), QUART)] + (tr[0, n] + tr[1, n])
        fin[4 * z + c] = res.astype(BF16)
        for j in (3, 2, 1):
            go(remote(fin.at[4 * z + c], fin.at[4 * z + c], f_s, f_r.at[n, j], dev_z[j]))
        go(remote(fin.at[4 * z + c], fin.at[4 * z + c], f_s, f_r.at[n, 0], dev_p))

    for c in range(4):
        yb[c] = cols(c)
        pl.when(k == 1 - c // 2)(lambda: e_copy(c).start())
        if c == 1:
            pl.when(k == 0)(lambda: pair(0))
        elif c == 2:
            pl.when(k == 0)(lambda: pair(1))
        elif c == 3:
            pl.when(k == 1)(lambda: pair(2))
    pl.when(k == 1)(lambda: pair(3))
    for n in range(2):
        finish(n)
    for n in range(2):
        for j in (1, 2, 3):
            at = fin.at[4 * zx[j] + 2 * k + n]
            remote(at, at, f_s, f_r.at[n, j], dev_p).wait_recv()
            go(remote(at, at, f_s, f_r.at[n, 3 + j], dev_p))
    for n in range(2):
        for j, zz in enumerate((z, zx[1], zx[2], zx[3])):
            at = fin.at[4 * zz + 2 * (1 - k) + n]
            remote(at, at, f_s, f_r.at[n, 3 + j if j else 0], dev_p).wait_recv()
    for i in range(4):
        for c in range(4):
            outf[4 * i:4 * i + 4, c * QUART:(c + 1) * QUART] = fin[4 * i + c].astype(F32)
    out_ref[...] = outf[...].astype(BF16)
    for src, sem in ((zq.at[pl.ds(0, 3)], q_s), (qg.at[:, 0], a_s.at[0]), (qg.at[:, 0], a_s.at[1]), (qg.at[:, 1], a_s.at[2]),
                     (acc.at[:, pl.ds(2, 2)], d_s), (acc.at[:, 1], y_s), (acc.at[pl.ds(0, 6), 0], z_s),
                     (yb.at[pl.ds(0, 2)], e_s), (tr.at[0], t_s), (fin.at[pl.ds(0, 14)], f_s)):
        remote(src, src, sem, d_r.at[0], dev_p).wait_send()


def solution(mesh):
    def local_step(hidden, lengths, latent_cache, rope_keys, w_uq, w_qr, w_uk, w_uv, w_out):
        rope_t = jnp.transpose(rope_keys, (0, 2, 1))
        wqr_t = jnp.transpose(w_qr, (1, 2, 0))
        anyspec = pl.BlockSpec(memory_space=pl.ANY)
        dma = pltpu.SemaphoreType.DMA
        scratch = [
            pltpu.VMEM((ROWS, D), BF16),
            pltpu.VMEM((ROWS, TLOC, LAT), BF16),
            pltpu.VMEM((ROWS, ROPE, TLOC), BF16),
            pltpu.VMEM((NCH // 2, 2 * CH, 4, NOPE), BF16),
            pltpu.VMEM((4, ROPE, D), BF16),
            pltpu.VMEM((HLOC, NOPE, LAT), BF16),
            pltpu.VMEM((HLOC, LAT, VAL), BF16),
            pltpu.VMEM((HLOC, VAL, D), BF16),
            pltpu.VMEM((48, 16, 512), BF16),
            pltpu.VMEM((4, 96, 128), BF16),
            pltpu.VMEM((HLOC, 16, QW), BF16),
            pltpu.VMEM((8, 4, 144, NOPE), BF16),
            pltpu.VMEM((2, 2, 64, TLOC), F32),
            pltpu.VMEM((8, 4, 136, 128), F32),
            pltpu.VMEM((8, 2, 136, 128), F32),
            pltpu.VMEM((8, 136, 128), F32),
            pltpu.VMEM((4, 2, 136, 128), F32),
            pltpu.VMEM((4, 4, QUART), F32),
            pltpu.VMEM((2, 4, QUART), F32),
            pltpu.VMEM((2, 2, 4, QUART), F32),
            pltpu.VMEM((16, 4, QUART), BF16),
            pltpu.VMEM((4, D), F32),
            pltpu.VMEM((ROWS, D), F32),
            dma((6,)), dma((2,)), dma,
            dma, dma((4,)),
            dma((3,)), dma((8, 3)),
            dma, dma((8,)),
            dma, dma((8,)),
            dma, dma((4, 2)),
            dma, dma((2,)), dma, dma((2,)),
            dma, dma((2, 7)),
        ]
        return pl.pallas_call(
            kernel,
            out_shape=pltpu.VMEM((ROWS, D), BF16),
            in_specs=[pl.BlockSpec(memory_space=pltpu.SMEM)] + [anyspec] * 8,
            out_specs=pl.BlockSpec(memory_space=pltpu.VMEM),
            scratch_shapes=scratch,
            compiler_params=pltpu.CompilerParams(collective_id=0, has_side_effects=True,
                                                 vmem_limit_bytes=66_000_000),
        )(lengths, hidden, latent_cache, rope_t, w_uq, wqr_t, w_uk, w_uv, w_out)

    row_spec, cache_spec = P('batch', None), P('batch', ('ctx', 'seq'), None)
    head_spec, proj_spec = P('seq', None, None), P(None, 'seq', None)
    return jax.shard_map(local_step, mesh=mesh,
                         in_specs=(row_spec, P('batch'), cache_spec, cache_spec, proj_spec, proj_spec, head_spec, head_spec, head_spec),
                         out_specs=row_spec, check_vma=False)
```

```python
import functools

import jax
import jax.numpy as jnp
from jax import lax
from jax.experimental import pallas as pl
from jax.experimental.pallas import tpu as pltpu
from jax.sharding import PartitionSpec as P

MESH = pl.DeviceIdType.MESH
F32, BF16 = jnp.float32, jnp.bfloat16
NEG = -3.0e38

ROWS, D, HLOC, NOPE, ROPE, LAT, VAL = 16, 6144, 16, 128, 64, 512, 128
TLOC = 512
QW = LAT + 128
CH = 1536
NCH = D // CH
BLK = CH // 128
QUART = D // 4
PAIR = 2
PACE = 1.2
LAG = 3.6
AHEAD = 5


def mm(a, b):
    return lax.dot_general(a, b, (((1,), (0,)), ((), ())), preferred_element_type=F32)


def mm_nt(a, b):
    return lax.dot_general(a, b, (((1,), (1,)), ((), ())), preferred_element_type=F32)


def onehot(shape, fn):
    i = lax.broadcasted_iota(jnp.int32, shape, 0)
    j = lax.broadcasted_iota(jnp.int32, shape, 1)
    return jnp.where(fn(i, j), 1.0, 0.0).astype(BF16)


def pack(ms, ls):
    lane = lax.broadcasted_iota(jnp.int32, (8, 128), 1)
    t = jnp.zeros((8, 128), F32)
    for i in range(2):
        for at, v in ((i, ms[i][0:8]), (2 + i, ms[i][8:16]), (4 + i, ls[i][0:8]), (6 + i, ls[i][8:16])):
            t = jnp.where(lane == at, v, t)
    return t


def unpack(t, i):
    return [jnp.concatenate([t[:, at + i:at + i + 1], t[:, at + 2 + i:at + 3 + i]], axis=0) for at in (0, 4)]


def merge(refs):
    out, nm, nl = [], [], []
    tiles = [r[128:136] for r in refs]
    for i in range(2):
        mls = [unpack(t, i) for t in tiles]
        m = functools.reduce(jnp.maximum, [v[0] for v in mls])
        fs = [jnp.exp(v[0] - m) for v in mls]
        nl.append(functools.reduce(jnp.add, [v[1] * f for v, f in zip(mls, fs)]))
        nm.append(m)
        for c in range(4):
            at = 16 * (4 * i + c)
            out.append(functools.reduce(jnp.add, [r[at:at + 16] * f for r, f in zip(refs, fs)]))
    return out, nm, nl


def kernel(len_ref, hid_hbm, cache_hbm, rope_hbm, wuq_hbm, wqr_hbm, wuk_hbm, wuv_hbm, wout_hbm, out_ref,
           hid, cache, rope, wuq, wqr, wuk, wuv, wout, rep, zq, xq, qg, sbuf, acc, racc, yra, zra,
           yb, yr, tr, fin, hsel, outf,
           lsem, usem, csem, q_s, q_r, a_s, a_r, d_s, d_r, y_s, y_r, z_s, z_r, e_s, e_r, t_s, t_r, f_s, f_r):
    x = lax.axis_index("batch")
    z = lax.axis_index("ctx")
    s = lax.axis_index("seq")
    y, k = s // 2, s % 2
    sp = s + 1 - 2 * k
    sy = s + 2 - 4 * y
    spy = sp + 2 - 4 * y
    zx = {1: z + 1 - 2 * (z % 2), 2: z + 2 - 4 * (z // 2), 3: 3 - z}
    inner = ((z + 1) // 2) % 2
    far = [3 * (1 - z // 2), 2 - z // 2]
    outer = 1 - inner
    gs = [inner * zx[1] + outer * far[0], inner * far[0] + outer * far[1], inner * far[1] + outer * zx[1], z]

    dev_p, dev_y = (x, z, sp), (x, z, sy)
    dev_z = {j: (x, zx[j], s) for j in zx}
    peers = [dev_p, dev_y, dev_z[1], dev_z[2], dev_z[3]]

    def local(src, dst, sem, priority=1):
        c = pltpu.make_async_copy(src, dst, sem)
        c.start(priority=priority)
        return c

    def remote(src, dst, ss, rs, dev):
        return pltpu.make_async_remote_copy(src_ref=src, dst_ref=dst, send_sem=ss, recv_sem=rs,
                                            device_id=dev, device_id_type=MESH)

    def go(c):
        c.start()

    own4 = pl.ds(pl.multiple_of(4 * z, 4), 4)
    c_hid = local(hid_hbm, hid, lsem.at[0], 0)

    def load_uq(i):
        return local(wuq_hbm.at[pl.ds(i * 2 * CH, 2 * CH), own4, :], wuq.at[i], usem.at[i])

    c_uq = [load_uq(i) for i in range(NCH // 2)]
    c_qr = local(wqr_hbm.at[own4], wqr, lsem.at[1])

    barrier = pltpu.get_barrier_semaphore()
    for d in peers:
        pl.semaphore_signal(barrier, inc=1, device_id=d, device_id_type=MESH)

    spread = onehot((128, 512), lambda i, j: j // 4 == i)
    lane = lax.broadcasted_iota(jnp.int32, (16, 128), 1)
    masks = [jnp.where(lane % 4 == h, 1.0, 0.0).astype(BF16) for h in range(4)]
    wide = [jnp.concatenate([m] * (CH * 4 // 128), axis=1) for m in masks]
    c_hid.wait()
    for t in range(NCH):
        blk = jnp.concatenate([hid[:, (BLK * t + i) * 128:(BLK * t + i + 1) * 128] for i in range(BLK)], axis=0)
        rep[pl.ds(BLK * t, BLK)] = mm(blk, spread).astype(BF16).reshape(BLK, 16, 512)
    qn = [jnp.zeros((64, NOPE), F32)] * 2
    for i in range(0, NCH, 2):
        c_uq[i // 2].wait()
        for part in range(2):
            for n in range(2):
                at, size = part * (BLK // 2), BLK // 2
                r = jnp.concatenate([rep[(i + n) * BLK + at + t] for t in range(size)], axis=1)
                lhs = jnp.concatenate([r * m[:, :size * 512] for m in wide], axis=0)
                qn[n] = qn[n] + mm(lhs, wuq[i // 2, (n * BLK + at) * 128:(n * BLK + at + size) * 128].reshape(size * 512, NOPE))
        if i == 0:
            c_uk = local(wuk_hbm, wuk, lsem.at[2])
    c_qr.wait()
    qr = jnp.concatenate([mm_nt(hid[...], wqr[2 * h:2 * h + 2].reshape(2 * ROPE, D)) for h in range(2)], axis=1)
    qr = qr.astype(BF16)
    zq[z, 64:80] = qr[:, :128]
    zq[z, 80:96] = qr[:, 128:]
    zq[z, 0:64] = (qn[0] + qn[1]).astype(BF16)
    c_rope = local(rope_hbm, rope, lsem.at[3])
    c_cache = local(cache_hbm, cache, csem)
    c_uv = local(wuv_hbm, wuv, lsem.at[4])
    c_out = local(wout_hbm, wout, lsem.at[5])

    pl.semaphore_wait(barrier, len(peers))
    def give_z():
        for j in (3, 2, 1):
            remote(zq.at[z], zq.at[z], q_s, q_r.at[z], dev_z[j]).start()

    give_z()
    pick = onehot((16, 16), lambda i, j: 4 * z + i == j)
    hsel[...] = mm(pick, hid[...])[0:4]

    def row_of(i):
        return sum((jnp.where(i // 4 == n, 4 * g, 0) for n, g in enumerate(gs))) + i % 4

    perm = onehot((256, 256), lambda i, j: (i % 16) * 16 + row_of(i // 16) == j)

    def latent(zz):
        for h in range(4):
            ql = mm(zq[zz, 16 * h:16 * h + 16], wuk[4 * zz + h]).astype(BF16)
            t = zq[zz, 64 + 16 * (h // 2):80 + 16 * (h // 2)]
            if h % 2:
                t = jnp.concatenate([t[:, 64:], t[:, :64]], axis=1)
            xq[4 * zz + h] = jnp.concatenate([ql, t], axis=1)

    c_uk.wait()
    latent(z)
    for j in (1, 2, 3):
        remote(zq.at[zx[j]], zq.at[zx[j]], q_s, q_r.at[zx[j]], dev_p).wait_recv()
        latent(zx[j])
    qp = mm(perm, xq[...].reshape(256, QW)).astype(BF16)
    def give(u):
        go(remote(qg.at[u, 0], qg.at[u, 1], a_s.at[0], a_r.at[u, 0], dev_y))
        go(remote(qg.at[u, 0], qg.at[u, 2], a_s.at[1], a_r.at[u, 1], dev_p))

    for u in range(8):
        rows = qp[32 * u:32 * u + 32]
        for c in range(4):
            qg[u, 0, 32 * c:32 * c + 32] = rows[:, NOPE * c:NOPE * c + NOPE]
        qg[u, 0, NOPE:] = jnp.concatenate([rows[:16, LAT:LAT + ROPE], rows[16:, LAT:LAT + ROPE]], axis=1)
        if u < AHEAD:
            give(u)

    def arrived(u, n):
        remote(qg.at[u, n], qg.at[u, n], a_s.at[0], a_r.at[u, n - 1], dev_p).wait_recv()

    def forward(u):
        arrived(u, 1)
        if u + AHEAD < 8:
            give(u + AHEAD)
        go(remote(qg.at[u, 1], qg.at[u, 3], a_s.at[2], a_r.at[u, 2], dev_p))

    scale = (NOPE + ROPE) ** -0.5
    t0 = (z * 4 + s) * TLOC

    def rows_of(u):
        return [4 * gs[u // PAIR] + 2 * (u % PAIR) + i for i in range(2)]

    def scores(u):
        for i, b in enumerate(rows_of(u)):
            q = [jnp.concatenate([qg[u, p, 32 * c + 16 * i:32 * c + 16 * i + 16] for p in range(4)], axis=0) for c in range(4)]
            r = jnp.concatenate([qg[u, p, NOPE:] for p in range(4)], axis=0)[:, ROPE * i:ROPE * i + ROPE]
            sbuf[u % PAIR, i] = mm_nt(jnp.concatenate(q, axis=1), cache[b]) + mm(r, rope[b])

    def attend(u):
        ws, ms, ls = [], [], []
        for i, b in enumerate(rows_of(u)):
            valid = lax.broadcasted_iota(jnp.int32, (64, TLOC), 1) < len_ref[b] - t0
            v = jnp.where(valid, sbuf[u % PAIR, i] * scale, NEG)
            m = jnp.max(v, axis=1, keepdims=True)
            w = jnp.where(valid, jnp.exp(v - m), 0.0)
            ms.append(m)
            ls.append(jnp.sum(w, axis=1, keepdims=True))
            ws.append(w.astype(BF16))
        for i, b in enumerate(rows_of(u)):
            o = mm(ws[i], cache[b])
            for p in range(4):
                for c in range(4):
                    acc[u, p, 16 * (4 * i + c):16 * (4 * i + c) + 16] = o[16 * p:16 * p + 16, 128 * c:128 * c + 128]
        for p in range(4):
            cut = slice(16 * p, 16 * p + 16)
            acc[u, p, 128:136] = pack([m[cut] for m in ms], [l[cut] for l in ls])

    def d_copy(u):
        return remote(acc.at[u, pl.ds(2, 2)], racc.at[u], d_s, d_r.at[u], dev_p)

    def y_copy(u):
        return remote(acc.at[u, 1], yra.at[u], y_s, y_r.at[u], dev_y)

    def z_copy(u):
        n, h = u // PAIR, u % PAIR
        to = inner * gs[n] + outer * zx[1]
        at = inner * (3 if n else 2) + outer * n
        return remote(acc.at[u, 0], zra.at[at, h], z_s, z_r.at[at, h], (x, to, s))

    def z_wait(at, h):
        remote(zra.at[at, h], zra.at[at, h], z_s, z_r.at[at, h], dev_p).wait_recv()

    def add(u, n, other):
        out, m, l = merge([acc[u, n], other])
        for c, o in enumerate(out):
            acc[u, n, 16 * c:16 * c + 16] = o
        acc[u, n, 128:136] = pack(m, l)

    def ready(u):
        arrived(u, 2)
        arrived(u, 3)
        if u < 7:
            forward(u + 1)
        scores(u)

    def stage_r(u):
        ready(u)

    def stage_a(u):
        if 1 < u < 7:
            ready(u + 1)
        attend(u)
        go(d_copy(u))

    def stage_y(u):
        d_copy(u).wait_recv()
        add(u, 1, racc[u, 1])
        go(y_copy(u))
        add(u, 0, racc[u, 0])

    def stage_z(u):
        if u == 5:
            pl.when(inner == 0)(lambda: z_copy(u - 1).start())
        y_copy(u).wait_recv()
        add(u, 0, yra[u])
        if u < 2:
            go(z_copy(u))
        elif u in (2, 3, 5):
            pl.when(inner == 0)(lambda: z_copy(u).start())

    def stage_c(u):
        @pl.when(inner == 1)
        def _():
            z_wait(u // PAIR - 1, u % PAIR)
            add(u, 0, zra[u // PAIR - 1, u % PAIR])
            z_copy(u).start()

    forward(0)
    c_rope.wait()
    c_cache.wait()
    plan = [(-1, stage_r, 0), (0.1, stage_r, 1), (0.4, stage_r, 2)]
    first = {(stage_a, 1): 0.2, (stage_y, 0): 0.3, (stage_y, 1): 0.5}
    for u in range(8):
        at = PACE * (u + 5) if u < 4 else 1.47 * u + 3.9
        plan += [(PACE * u, stage_a, u), (PACE * (u + 1) + (0.1 if u else -0.9), stage_y, u), (at, stage_z, u)]
        if u < 4:
            plan.append((at + LAG, stage_c, u + 2))
    for _, stage, u in sorted(plan, key=lambda e: first.get(e[1:], e[0])):
        stage(u)

    c_uv.wait()
    c_out.wait()
    ol = []
    for h in range(2):
        u = 6 + h
        z_wait(2, h)
        z_wait(3, h)
        if h:
            pass
        out, m, l = merge([acc[u, 0], zra[2, h], zra[3, h]])
        ol += [jnp.concatenate([(out[4 * i + c] / l[i]).astype(BF16) for c in range(4)], axis=1) for i in range(2)]
    ol = jnp.concatenate(ol, axis=0)
    vs = []
    head = lax.broadcasted_iota(jnp.int32, (64, VAL), 0) % 16
    for h in range(HLOC):
        vs.append(jnp.where(head == h, mm(ol, wuv[h]), 0.0).astype(BF16))
    v = jnp.concatenate(vs, axis=1)
    fold = onehot((16, 64), lambda i, j: j // 16 == i)
    v = mm(fold, v).astype(BF16)

    def cols(c):
        return mm(v, wout[:, :, c * QUART:(c + 1) * QUART].reshape(HLOC * VAL, QUART))[0:4]

    def e_copy(c):
        return remote(yb.at[c], yr.at[c % 2], e_s, e_r.at[c % 2], dev_p)

    def t_copy(n):
        return remote(tr.at[0, n], tr.at[1, n], t_s, t_r.at[n], dev_y)

    def pair(c):
        n = c % 2
        e_copy(c).wait_recv()
        tr[0, n] = yb[c] + yr[n]
        t_copy(n).start()

    def finish(n):
        t_copy(n).wait_recv()
        c = 2 * k + n
        res = hsel[:, pl.ds(pl.multiple_of(c * QUART, QUART), QUART)] + (tr[0, n] + tr[1, n])
        fin[4 * z + c] = res.astype(BF16)
        for j in (3, 2, 1):
            go(remote(fin.at[4 * z + c], fin.at[4 * z + c], f_s, f_r.at[n, j], dev_z[j]))
        go(remote(fin.at[4 * z + c], fin.at[4 * z + c], f_s, f_r.at[n, 0], dev_p))

    for c in range(4):
        yb[c] = cols(c)
        pl.when(k == 1 - c // 2)(lambda: e_copy(c).start())
        if c == 1:
            pl.when(k == 0)(lambda: pair(0))
        elif c == 2:
            pl.when(k == 0)(lambda: pair(1))
        elif c == 3:
            pl.when(k == 1)(lambda: pair(2))
    pl.when(k == 1)(lambda: pair(3))
    for n in range(2):
        finish(n)
    for n in range(2):
        for j in (1, 2, 3):
            at = fin.at[4 * zx[j] + 2 * k + n]
            remote(at, at, f_s, f_r.at[n, j], dev_p).wait_recv()
            go(remote(at, at, f_s, f_r.at[n, 3 + j], dev_p))
    for n in range(2):
        for j, zz in enumerate((z, zx[1], zx[2], zx[3])):
            at = fin.at[4 * zz + 2 * (1 - k) + n]
            remote(at, at, f_s, f_r.at[n, 3 + j if j else 0], dev_p).wait_recv()
    for i in range(4):
        for c in range(4):
            outf[4 * i:4 * i + 4, c * QUART:(c + 1) * QUART] = fin[4 * i + c].astype(F32)
    out_ref[...] = outf[...].astype(BF16)
    for src, sem in ((zq.at[pl.ds(0, 3)], q_s), (qg.at[:, 0], a_s.at[0]), (qg.at[:, 0], a_s.at[1]), (qg.at[:, 1], a_s.at[2]),
                     (acc.at[:, pl.ds(2, 2)], d_s), (acc.at[:, 1], y_s), (acc.at[pl.ds(0, 6), 0], z_s),
                     (yb.at[pl.ds(0, 2)], e_s), (tr.at[0], t_s), (fin.at[pl.ds(0, 14)], f_s)):
        remote(src, src, sem, d_r.at[0], dev_p).wait_send()


def solution(mesh):
    def local_step(hidden, lengths, latent_cache, rope_keys, w_uq, w_qr, w_uk, w_uv, w_out):
        rope_t = jnp.transpose(rope_keys, (0, 2, 1))
        wqr_t = jnp.transpose(w_qr, (1, 2, 0))
        anyspec = pl.BlockSpec(memory_space=pl.ANY)
        dma = pltpu.SemaphoreType.DMA
        scratch = [
            pltpu.VMEM((ROWS, D), BF16),
            pltpu.VMEM((ROWS, TLOC, LAT), BF16),
            pltpu.VMEM((ROWS, ROPE, TLOC), BF16),
            pltpu.VMEM((NCH // 2, 2 * CH, 4, NOPE), BF16),
            pltpu.VMEM((4, ROPE, D), BF16),
            pltpu.VMEM((HLOC, NOPE, LAT), BF16),
            pltpu.VMEM((HLOC, LAT, VAL), BF16),
            pltpu.VMEM((HLOC, VAL, D), BF16),
            pltpu.VMEM((48, 16, 512), BF16),
            pltpu.VMEM((4, 96, 128), BF16),
            pltpu.VMEM((HLOC, 16, QW), BF16),
            pltpu.VMEM((8, 4, 144, NOPE), BF16),
            pltpu.VMEM((2, 2, 64, TLOC), F32),
            pltpu.VMEM((8, 4, 136, 128), F32),
            pltpu.VMEM((8, 2, 136, 128), F32),
            pltpu.VMEM((8, 136, 128), F32),
            pltpu.VMEM((4, 2, 136, 128), F32),
            pltpu.VMEM((4, 4, QUART), F32),
            pltpu.VMEM((2, 4, QUART), F32),
            pltpu.VMEM((2, 2, 4, QUART), F32),
            pltpu.VMEM((16, 4, QUART), BF16),
            pltpu.VMEM((4, D), F32),
            pltpu.VMEM((ROWS, D), F32),
            dma((6,)), dma((2,)), dma,
            dma, dma((4,)),
            dma((3,)), dma((8, 3)),
            dma, dma((8,)),
            dma, dma((8,)),
            dma, dma((4, 2)),
            dma, dma((2,)), dma, dma((2,)),
            dma, dma((2, 7)),
        ]
        return pl.pallas_call(
            kernel,
            out_shape=pltpu.VMEM((ROWS, D), BF16),
            in_specs=[pl.BlockSpec(memory_space=pltpu.SMEM)] + [anyspec] * 8,
            out_specs=pl.BlockSpec(memory_space=pltpu.VMEM),
            scratch_shapes=scratch,
            compiler_params=pltpu.CompilerParams(collective_id=0, has_side_effects=True,
                                                 vmem_limit_bytes=66_000_000),
        )(lengths, hidden, latent_cache, rope_t, w_uq, wqr_t, w_uk, w_uv, w_out)

    row_spec, cache_spec = P('batch', None), P('batch', ('ctx', 'seq'), None)
    head_spec, proj_spec = P('seq', None, None), P(None, 'seq', None)
    return jax.shard_map(local_step, mesh=mesh,
                         in_specs=(row_spec, P('batch'), cache_spec, cache_spec, proj_spec, proj_spec, head_spec, head_spec, head_spec),
                         out_specs=row_spec, check_vma=False)
```
